128 devices in a mesh: z: 4 (over z), y: 4 (over y), x: 8 (over x, core).
Axes of the slice: x: 4, y: 4, z: 4, core: 2. Of those that a mesh axis runs over, the one named last changes fastest.
Arguments:
- acts_in: bfloat16 [262144, 512], P(('z', 'y', 'x'))
- grad_out: bfloat16 [262144, 512], P(('z', 'y', 'x'))
- w_up1: bfloat16 [512, 2048], replicated
- w_down1: bfloat16 [2048, 512], replicated
- w_up2: bfloat16 [512, 2048], replicated
- w_down2: bfloat16 [2048, 512], replicated
Outputs:
- output 1: float32 [512, 2048], replicated
- output 2: float32 [2048, 512], replicated
- output 3: float32 [512, 2048], replicated
- output 4: float32 [2048, 512], replicated
- output 5: bfloat16 [262144, 512], P(('z', 'y', 'x'))
All inputs are finite; a program needn't handle non-finite values.
Results may differ from the reference program's by a relative error of at most 0.0134572.
Values are sent between devices in bfloat16 or wider.
A program may use at most 1 GiB of HBM per device.

```python
import jax
import jax.numpy as jnp
from jax import lax
import math

TOK_DEV = 2048
N_DEVICES = 128
D_MODEL = 512
D_FF = 2048
N_TOKENS = TOK_DEV * N_DEVICES
INV_ROOT_TWO = 1.0 / math.sqrt(2.0)
INV_ROOT_TWO_PI = 1.0 / math.sqrt(2.0 * math.pi)


def setup_inputs(seed: int = 0) -> dict:
    key_list = jax.random.split(jax.random.key(seed), 6)
    acts_in = jax.random.normal(key_list[0], (N_TOKENS, D_MODEL), jnp.float32)
    grad_out = jax.random.normal(key_list[1], (N_TOKENS, D_MODEL), jnp.float32)
    w_up1 = jax.random.normal(key_list[2], (D_MODEL, D_FF), jnp.float32) * D_MODEL ** -0.5
    w_down1 = jax.random.normal(key_list[3], (D_FF, D_MODEL), jnp.float32) * D_FF ** -0.5
    w_up2 = jax.random.normal(key_list[4], (D_MODEL, D_FF), jnp.float32) * D_MODEL ** -0.5
    w_down2 = jax.random.normal(key_list[5], (D_FF, D_MODEL), jnp.float32) * D_FF ** -0.5
    return dict(acts_in=acts_in.astype(jnp.bfloat16), grad_out=grad_out.astype(jnp.bfloat16), w_up1=w_up1.astype(jnp.bfloat16), w_down1=w_down1.astype(jnp.bfloat16), w_up2=w_up2.astype(jnp.bfloat16), w_down2=w_down2.astype(jnp.bfloat16))


def gelu_slope(pre_act):
    return 0.5 * (1.0 + lax.erf(pre_act * INV_ROOT_TWO)) + pre_act * jnp.exp(-0.5 * pre_act * pre_act) * INV_ROOT_TWO_PI


def device_grads(acts_local, grad_top, w_up1, w_down1, w_up2, w_down2):
    pre_one = jnp.dot(acts_local, w_up1, preferred_element_type=jnp.float32).astype(jnp.bfloat16)
    hid_one = jax.nn.gelu(pre_one.astype(jnp.float32), approximate=False).astype(jnp.bfloat16)
    mid_res = (jnp.dot(hid_one, w_down1, preferred_element_type=jnp.float32) + acts_local.astype(jnp.float32)).astype(jnp.bfloat16)
    pre_two = jnp.dot(mid_res, w_up2, preferred_element_type=jnp.float32).astype(jnp.bfloat16)
    hid_two = jax.nn.gelu(pre_two.astype(jnp.float32), approximate=False).astype(jnp.bfloat16)
    gw_down2 = jnp.dot(hid_two.T, grad_top, preferred_element_type=jnp.float32)
    grad_hid2 = jnp.dot(grad_top, w_down2.T, preferred_element_type=jnp.float32).astype(jnp.bfloat16)
    grad_pre2 = (grad_hid2.astype(jnp.float32) * gelu_slope(pre_two.astype(jnp.float32))).astype(jnp.bfloat16)
    gw_up2 = jnp.dot(mid_res.T, grad_pre2, preferred_element_type=jnp.float32)
    grad_mid = (jnp.dot(grad_pre2, w_up2.T, preferred_element_type=jnp.float32) + grad_top.astype(jnp.float32)).astype(jnp.bfloat16)
    gw_down1 = jnp.dot(hid_one.T, grad_mid, preferred_element_type=jnp.float32)
    grad_hid1 = jnp.dot(grad_mid, w_down1.T, preferred_element_type=jnp.float32).astype(jnp.bfloat16)
    grad_pre1 = (grad_hid1.astype(jnp.float32) * gelu_slope(pre_one.astype(jnp.float32))).astype(jnp.bfloat16)
    gw_up1 = jnp.dot(acts_local.T, grad_pre1, preferred_element_type=jnp.float32)
    grad_acts = (jnp.dot(grad_pre1, w_up1.T, preferred_element_type=jnp.float32) + grad_mid.astype(jnp.float32)).astype(jnp.bfloat16)
    return (gw_up1, gw_down1, gw_up2, gw_down2), grad_acts


def reference(acts_in, grad_out, w_up1, w_down1, w_up2, w_down2):
    acts_blocks = acts_in.reshape(N_DEVICES, TOK_DEV, D_MODEL)
    grad_blocks = grad_out.reshape(N_DEVICES, TOK_DEV, D_MODEL)
    zero_sums = (jnp.zeros((D_MODEL, D_FF), jnp.float32), jnp.zeros((D_FF, D_MODEL), jnp.float32), jnp.zeros((D_MODEL, D_FF), jnp.float32), jnp.zeros((D_FF, D_MODEL), jnp.float32))

    def scan_step(run_sums, block_pair):
        local_grads, grad_acts = device_grads(block_pair[0], block_pair[1], w_up1, w_down1, w_up2, w_down2)
        new_sums = tuple(part_sum + local_grad for part_sum, local_grad in zip(run_sums, local_grads))
        return new_sums, grad_acts

    run_sums, grad_in_blocks = lax.scan(scan_step, zero_sums, (acts_blocks, grad_blocks))
    return (run_sums[0] / N_DEVICES, run_sums[1] / N_DEVICES, run_sums[2] / N_DEVICES, run_sums[3] / N_DEVICES, grad_in_blocks.reshape(N_TOKENS, D_MODEL))
```

```python
import math
import jax
import jax.numpy as jnp
from jax import lax
from jax.sharding import PartitionSpec as P

INV_ROOT_TWO = 1.0 / math.sqrt(2.0)
INV_ROOT_TWO_PI = 1.0 / math.sqrt(2.0 * math.pi)
ROW_CONTRACT = (((0,), (0,)), ((), ()))
COL_CONTRACT = (((1,), (1,)), ((), ()))


def gelu(pre_act):
    return 0.5 * pre_act * (1.0 + lax.erf(pre_act * INV_ROOT_TWO))


def gelu_slope(pre_act):
    return 0.5 * (1.0 + lax.erf(pre_act * INV_ROOT_TWO)) + pre_act * jnp.exp(-0.5 * pre_act * pre_act) * INV_ROOT_TWO_PI


def matmul(lhs, rhs):
    return jnp.dot(lhs, rhs, preferred_element_type=jnp.float32)


def contract(lhs, rhs, dims):
    return lax.dot_general(lhs, rhs, dims, preferred_element_type=jnp.float32)


def local_backward(acts_local, grad_top, w_up1, w_down1, w_up2, w_down2, reduce_fn):
    pre_one = matmul(acts_local, w_up1).astype(jnp.bfloat16)
    hid_one = gelu(pre_one.astype(jnp.float32)).astype(jnp.bfloat16)
    mid_res = (matmul(hid_one, w_down1) + acts_local.astype(jnp.float32)).astype(jnp.bfloat16)
    pre_two = matmul(mid_res, w_up2).astype(jnp.bfloat16)
    hid_two = gelu(pre_two.astype(jnp.float32)).astype(jnp.bfloat16)
    gw_down2 = reduce_fn(contract(hid_two, grad_top, ROW_CONTRACT))
    grad_hid2 = contract(grad_top, w_down2, COL_CONTRACT).astype(jnp.bfloat16)
    grad_pre2 = (grad_hid2.astype(jnp.float32) * gelu_slope(pre_two.astype(jnp.float32))).astype(jnp.bfloat16)
    gw_up2 = reduce_fn(contract(mid_res, grad_pre2, ROW_CONTRACT))
    grad_mid = (contract(grad_pre2, w_up2, COL_CONTRACT) + grad_top.astype(jnp.float32)).astype(jnp.bfloat16)
    gw_down1 = reduce_fn(contract(hid_one, grad_mid, ROW_CONTRACT))
    grad_hid1 = contract(grad_mid, w_down1, COL_CONTRACT).astype(jnp.bfloat16)
    grad_pre1 = (grad_hid1.astype(jnp.float32) * gelu_slope(pre_one.astype(jnp.float32))).astype(jnp.bfloat16)
    gw_up1 = reduce_fn(contract(acts_local, grad_pre1, ROW_CONTRACT))
    grad_acts = (contract(grad_pre1, w_up1, COL_CONTRACT) + grad_mid.astype(jnp.float32)).astype(jnp.bfloat16)
    return (gw_up1, gw_down1, gw_up2, gw_down2, grad_acts)


def solution(mesh):
    n_dev = math.prod(mesh.shape.values())
    batch_spec = P(('z', 'y', 'x'), None)
    full_spec = P(None, None)

    def reduce_grad(local_grad):
        return lax.psum(local_grad, ('z', 'y', 'x')) / n_dev

    def per_device(acts_in, grad_out, w_up1, w_down1, w_up2, w_down2):
        return local_backward(acts_in, grad_out, w_up1, w_down1, w_up2, w_down2, reduce_grad)

    return jax.shard_map(per_device, mesh=mesh, in_specs=(batch_spec, batch_spec, full_spec, full_spec, full_spec, full_spec), out_specs=(full_spec, full_spec, full_spec, full_spec, batch_spec), check_vma=False)
```

```python
import functools
import math
import jax
import jax.numpy as jnp
from jax import lax
from jax.experimental import pallas as pl
from jax.experimental.pallas import tpu as pltpu
from jax.sharding import PartitionSpec as P

INV_ROOT_TWO = 1.0 / math.sqrt(2.0)
INV_ROOT_TWO_PI = 1.0 / math.sqrt(2.0 * math.pi)
MESH = pl.DeviceIdType.MESH
BF16 = jnp.bfloat16
F32 = jnp.float32

TOK, DM, FF = 2048, 512, 2048
NB = 4
CB = FF // NB
NQ = 2 * NB
TT = 512
NT = TOK // TT
ND = 5
ROWS = (128, 32, 8)
GROUPS = ((0, 2), (2, 1), (3, 1))
OFFS = ((0, 128, 256), (384, 416, 448), (480, 488, 496))


def dot_nn(a, b):
    return lax.dot_general(a, b, (((1,), (0,)), ((), ())), preferred_element_type=F32)


def dot_nt(a, b):
    return lax.dot_general(a, b, (((1,), (1,)), ((), ())), preferred_element_type=F32)


def dot_tn(a, b):
    return lax.dot_general(a, b, (((0,), (0,)), ((), ())), preferred_element_type=F32)


def gelu_and_slope(pre):
    cdf = 0.5 * (1.0 + lax.erf(pre * INV_ROOT_TWO))
    return pre * cdf, cdf + pre * jnp.exp(-0.5 * pre * pre) * INV_ROOT_TWO_PI


def gelu(pre):
    return pre * (0.5 * (1.0 + lax.erf(pre * INV_ROOT_TWO)))


def kernel(x_hbm, g_hbm, w1_hbm, w2_hbm, w3_hbm, w4_hbm,
           o1, o2, o3, o4, odx,
           xv, gv, w1, w2, w3, w4, a1, h2, dh2, da, hc,
           gb, drb, rbuf,
           in_sem, rsem, ssem, dsem_s, dsem_r, osem, xsem):
    z, y, x = lax.axis_index('z'), lax.axis_index('y'), lax.axis_index('x')
    core = lax.rem(x, 2)
    cx = lax.div(x, 2)
    partner = (z, y, x + 1 - 2 * core)

    def hot(d):
        return lax.div((2 - d) * (1 - d), 2), d * (2 - d), lax.div(d * (d - 1), 2)

    def pos(d):
        ox, oy, oz = hot(d)
        return cx * ox + y * oy + z * oz

    def nbr(d, e):
        ox, oy, oz = hot(d)
        return (lax.rem(z + e * oz + 4, 4), lax.rem(y + e * oy + 4, 4),
                lax.rem(cx + e * ox + 4, 4) * 2 + core)

    loads = []
    n = 0

    def load(src, dst):
        nonlocal n
        cp = pltpu.make_async_copy(src, dst, in_sem.at[n])
        cp.start()
        n += 1
        return cp

    ld_x = load(x_hbm, xv)
    ld_w1 = [load(w1_hbm.at[:, pl.ds(c * CB, CB)], w1.at[c]) for c in range(NB)]
    ld_w2 = [load(w2_hbm.at[pl.ds(c * CB, CB), :], w2.at[c]) for c in range(NB)]
    ld_w3 = [load(w3_hbm.at[:, pl.ds(c * CB, CB)], w3.at[c]) for c in range(NB)]
    ld_g = load(g_hbm, gv)
    ld_w4 = [load(w4_hbm.at[pl.ds(c * CB, CB), :], w4.at[c]) for c in range(NB)]

    barrier = pltpu.get_barrier_semaphore()
    peers = [partner] + [nbr(d, e) for d in range(3) for e in (1, -1)]
    for peer in peers:
        pl.semaphore_signal(barrier, inc=1, device_id=peer, device_id_type=MESH)
    pl.semaphore_wait(barrier, len(peers))

    ld_x.wait()
    for cp in ld_w1 + ld_w2:
        cp.wait()

    def fwd1(t, carry):
        rows = pl.ds(pl.multiple_of(t * TT, TT), TT)
        xt = xv[rows, :]
        acc = xt.astype(F32)
        for c in range(NB):
            pre = dot_nn(xt, w1[c]).astype(BF16)
            a1[c, rows, :] = pre
            acc = acc + dot_nn(gelu(pre.astype(F32)).astype(BF16), w2[c])
        h2[rows, :] = acc.astype(BF16)
        return carry

    lax.fori_loop(0, NT, fwd1, 0)
    for cp in ld_w3 + [ld_g] + ld_w4:
        cp.wait()

    def group(q, gi):
        u0, s = GROUPS[gi]
        rot = lax.rem(q + gi, 3)
        e = 1 - 2 * lax.rem(q + gi, 2)
        dims = [lax.rem(rot + k, 3) for k in range(3)]
        ps = [pos(d) for d in dims]
        base = [0, ps[0] * ROWS[0], ps[0] * ROWS[0] + ps[1] * ROWS[1]]
        return u0, s, e, dims, ps, base

    def piece(q, half, u0, s, start, length):
        return gb.at[q, half, pl.ds(u0, s), pl.ds(pl.multiple_of(start, 8), length), :]

    def rb(slot, u0, s, off, length):
        return rbuf.at[slot, pl.ds(u0, s), pl.ds(off, length), :]

    class Phase:
        def __init__(self, q, gi, k):
            self.u0, self.s, self.e, dims, ps, base = group(q, gi)
            self.q, self.gi, self.k = q, gi, k
            self.d, self.p, self.base = dims[k], ps[k], base[k]
            self.L = ROWS[k]
            self.slot = lax.rem(q, 2)
            self.dslot = lax.rem(q, ND)

        def rows(self, j):
            return self.base + lax.rem(self.p + j + 4, 4) * self.L

        def mine(self, j):
            return piece(self.q, core, self.u0, self.s, self.rows(j), self.L)

        def part(self, j):
            return drb.at[self.dslot, pl.ds(self.u0, self.s), pl.ds(pl.multiple_of(self.rows(j), 8), self.L), :]

        def pval(self, j):
            return (self.dslot, pl.ds(self.u0, self.s), pl.ds(pl.multiple_of(self.rows(j), 8), self.L), slice(None))

        def val(self, j):
            return (self.q, core, pl.ds(self.u0, self.s), pl.ds(pl.multiple_of(self.rows(j), 8), self.L), slice(None))

        def buf(self, i):
            return rb(self.slot, self.u0, self.s, OFFS[self.k][i], self.L)

        def bufval(self, i):
            return rbuf[self.slot, pl.ds(self.u0, self.s), pl.ds(OFFS[self.k][i], self.L), :]

        def copy(self, src, dst, i, toward):
            idx = self.k * 6 + i
            return pltpu.make_async_remote_copy(
                src_ref=src, dst_ref=dst, send_sem=ssem.at[self.slot, self.gi, idx],
                recv_sem=rsem.at[self.slot, self.gi, idx],
                device_id=nbr(self.d, toward), device_id_type=MESH)

        def far(self):
            return self.copy(self.part(2), self.buf(0), 0, self.e)

        def near(self):
            return self.copy(self.part(-self.e), self.buf(1), 1, -self.e)

        def comb(self):
            return self.copy(self.part(self.e), self.buf(2), 2, self.e)

        def own_fwd(self):
            return self.copy(self.mine(0), self.mine(0), 3, self.e)

        def own_bwd(self):
            return self.copy(self.mine(0), self.mine(0), 4, -self.e)

        def relay(self):
            return self.copy(self.mine(-self.e), self.mine(-self.e), 5, self.e)

    def rs_a(q, k):
        for gi in range(3):
            ph = Phase(q, gi, k)
            ph.far().start()
            ph.near().start()

    def rs_b(q, k):
        for gi in range(3):
            ph = Phase(q, gi, k)
            ph.far().wait_recv()
            ix = ph.pval(ph.e)
            drb[ix] = drb[ix] + ph.bufval(0)
            ph.comb().start()

    def rs_c(q, k):
        for gi in range(3):
            ph = Phase(q, gi, k)
            ph.near().wait_recv()
            ph.comb().wait_recv()
            ix = ph.pval(0)
            tot = drb[ix] + (ph.bufval(1) + ph.bufval(2))
            if k == 2:
                gb[ph.val(0)] = tot * (1.0 / 128.0)
            else:
                drb[ix] = tot
            ph.far().wait_send()
            ph.near().wait_send()
            ph.comb().wait_send()

    def ag_a(q, k):
        for gi in range(3):
            ph = Phase(q, gi, k)
            ph.own_fwd().start()
            ph.own_bwd().start()

    def ag_b(q, k):
        for gi in range(3):
            ph = Phase(q, gi, k)
            ph.own_fwd().wait_recv()
            ph.relay().start()

    def ag_c(q, k):
        for gi in range(3):
            ph = Phase(q, gi, k)
            ph.own_bwd().wait_recv()
            ph.relay().wait_recv()
            ph.own_fwd().wait_send()
            ph.own_bwd().wait_send()
            ph.relay().wait_send()

    def d2d(q, back):
        slot = lax.rem(q, 2)
        if back:
            src = dst = gb.at[q, core]
        else:
            src, dst = gb.at[q, 1 - core], drb.at[lax.rem(q, ND)]
        return pltpu.make_async_remote_copy(
            src_ref=src, dst_ref=dst, send_sem=dsem_s.at[slot, int(back)], recv_sem=dsem_r.at[slot, int(back)],
            device_id=partner, device_id_type=MESH)

    def outs(q, act):
        slot = lax.rem(q, 2)

        def move(down, up, c):
            for half in range(2):
                for u in range(4):
                    src = gb.at[q, half, u]
                    if half == 0:
                        dst = down.at[pl.ds(pl.multiple_of(c * CB, CB), CB), pl.ds(u * 128, 128)]
                    else:
                        dst = up.at[:, pl.ds(pl.multiple_of(c * CB + u * 128, 128), 128)]
                    act(pltpu.make_async_copy(src, dst, osem.at[slot, half * 4 + u]))

        @pl.when(q < NB)
        def _():
            move(o4, o3, q)

        @pl.when(q >= NB)
        def _():
            move(o2, o1, q - NB)

    def stage(s, q):
        if s == 0:
            d2d(q, False).start()
        elif s == 1:
            d2d(q, False).wait_recv()
            slot = lax.rem(q, ND)
            drb[slot] = gb[q, core] + drb[slot]
            d2d(q, False).wait_send()
            rs_a(q, 0)
        elif s == 2:
            rs_b(q, 0)
        elif s == 3:
            rs_c(q, 0)
            rs_a(q, 1)
        elif s == 4:
            rs_b(q, 1)
        elif s == 5:
            rs_c(q, 1)
            rs_a(q, 2)
        elif s == 6:
            rs_b(q, 2)
        elif s == 7:
            rs_c(q, 2)
            ag_a(q, 2)
        elif s == 8:
            ag_b(q, 2)
        elif s == 9:
            ag_c(q, 2)
            ag_a(q, 1)
        elif s == 10:
            ag_b(q, 1)
        elif s == 11:
            ag_c(q, 1)
            ag_a(q, 0)
        elif s == 12:
            ag_b(q, 0)
        elif s == 13:
            ag_c(q, 0)
            d2d(q, True).start()
        elif s == 14:
            d2d(q, True).wait_recv()
            d2d(q, True).wait_send()
            outs(q, lambda cp: cp.start())
        elif s == 15:
            outs(q, lambda cp: cp.wait())

    def tick(i, odd):
        top = 15 if odd else 14
        for s in range(top, -1, -2):
            q = i - (s + 1) // 2

            @pl.when((q >= 0) & (q < NQ))
            def _():
                stage(s, q)

    def tile2(c):
        def body(t, carry):
            rows = pl.ds(pl.multiple_of(t * TT, TT), TT)
            pre = dot_nn(h2[rows, :], w3[c]).astype(BF16).astype(F32)
            act, slope = gelu_and_slope(pre)
            hc[rows, :] = act.astype(BF16)
            up = dot_nt(gv[rows, :], w4[c]).astype(BF16).astype(F32)
            da[c, rows, :] = (up * slope).astype(BF16)
            return carry
        lax.fori_loop(0, NT, body, 0)

    def tile1(c):
        def body(t, carry):
            rows = pl.ds(pl.multiple_of(t * TT, TT), TT)
            pre = a1[c, rows, :].astype(F32)
            act, slope = gelu_and_slope(pre)
            hc[rows, :] = act.astype(BF16)
            up = dot_nt(dh2[rows, :], w2[c]).astype(BF16).astype(F32)
            da[c, rows, :] = (up * slope).astype(BF16)
            return carry
        lax.fori_loop(0, NT, body, 0)

    def wgrad(q, c, down_rhs, up_lhs):
        down = dot_tn(hc[...], down_rhs[...])
        for u in range(4):
            gb[q, 0, u] = down[:, u * 128:(u + 1) * 128]
        up = dot_tn(up_lhs[...], da[c])
        for u in range(4):
            gb[q, 1, u] = up[:, u * 128:(u + 1) * 128]

    def back_tile(t, w, res, dst):
        rows = pl.ds(pl.multiple_of(t * TT, TT), TT)
        acc = res[rows, :].astype(F32)
        for c in range(NB):
            acc = acc + dot_nt(da[c, rows, :], w[c])
        dst[rows, :] = acc.astype(BF16)

    def step(i, carry):
        @pl.when(i < NB)
        def _():
            tile2(i)

        @pl.when(i == NB)
        def _():
            def body(t, c):
                back_tile(t, w3, gv, dh2)
                return c
            lax.fori_loop(0, NT, body, 0)

        @pl.when((i >= NB) & (i < NQ))
        def _():
            tile1(i - NB)

        @pl.when((i >= NQ) & (i < NQ + NT))
        def _():
            back_tile(i - NQ, w1, dh2, h2)

        tick(i, True)

        @pl.when(i < NB)
        def _():
            wgrad(i, i, gv, h2)

        @pl.when((i >= NB) & (i < NQ))
        def _():
            wgrad(i, i - NB, dh2, xv)

        @pl.when(i == NQ + NT)
        def _():
            pltpu.make_async_copy(h2, odx, xsem).start()

        tick(i, False)
        return carry

    lax.fori_loop(0, 2 * NQ, step, 0)
    pltpu.make_async_copy(h2, odx, xsem).wait()


def solution(mesh):
    batch_spec = P(('z', 'y', 'x'), None)
    full_spec = P(None, None)

    def per_device(acts_in, grad_out, w_up1, w_down1, w_up2, w_down2):
        any_spec = pl.BlockSpec(memory_space=pl.ANY)
        up = jax.ShapeDtypeStruct((DM, FF), F32)
        down = jax.ShapeDtypeStruct((FF, DM), F32)
        return pl.pallas_call(
            kernel,
            out_shape=(up, down, up, down, jax.ShapeDtypeStruct((TOK, DM), BF16)),
            in_specs=[any_spec] * 6,
            out_specs=(any_spec,) * 5,
            scratch_shapes=[
                pltpu.VMEM((TOK, DM), BF16),
                pltpu.VMEM((TOK, DM), BF16),
                pltpu.VMEM((NB, DM, CB), BF16),
                pltpu.VMEM((NB, CB, DM), BF16),
                pltpu.VMEM((NB, DM, CB), BF16),
                pltpu.VMEM((NB, CB, DM), BF16),
                pltpu.VMEM((NB, TOK, CB), BF16),
                pltpu.VMEM((TOK, DM), BF16),
                pltpu.VMEM((TOK, DM), BF16),
                pltpu.VMEM((NB, TOK, CB), BF16),
                pltpu.VMEM((TOK, CB), BF16),
                pltpu.VMEM((NQ, 2, 4, 512, 128), F32),
                pltpu.VMEM((ND, 4, 512, 128), F32),
                pltpu.VMEM((2, 4, 504, 128), F32),
                pltpu.SemaphoreType.DMA((18,)),
                pltpu.SemaphoreType.DMA((2, 3, 18)),
                pltpu.SemaphoreType.DMA((2, 3, 18)),
                pltpu.SemaphoreType.DMA((2, 2)),
                pltpu.SemaphoreType.DMA((2, 2)),
                pltpu.SemaphoreType.DMA((2, 8)),
                pltpu.SemaphoreType.DMA,
            ],
            compiler_params=pltpu.CompilerParams(
                collective_id=0, has_side_effects=True, vmem_limit_bytes=67043328),
            cost_estimate=pl.CostEstimate(flops=12 * 2 * TOK * DM * FF, bytes_accessed=32 * 2**20, transcendentals=0),
        )(acts_in, grad_out, w_up1, w_down1, w_up2, w_down2)

    return jax.shard_map(per_device, mesh=mesh, in_specs=(batch_spec, batch_spec, full_spec, full_spec, full_spec, full_spec), out_specs=(full_spec, full_spec, full_spec, full_spec, batch_spec), check_vma=False)
```

```python
import functools
import math
import jax
import jax.numpy as jnp
from jax import lax
from jax.experimental import pallas as pl
from jax.experimental.pallas import tpu as pltpu
from jax.sharding import PartitionSpec as P

INV_ROOT_TWO = 1.0 / math.sqrt(2.0)
INV_ROOT_TWO_PI = 1.0 / math.sqrt(2.0 * math.pi)
MESH = pl.DeviceIdType.MESH
BF16 = jnp.bfloat16
F32 = jnp.float32

TOK, DM, FF = 2048, 512, 2048
NB = 4
CB = FF // NB
NQ = 2 * NB
TT = 512
NT = TOK // TT
ND = 6
SL = 3
PER, DIST = 3, 2
DIRECT = (False, True, True)
ROWS = (128, 32, 8)
GROUPS = ((0, 2), (2, 1), (3, 1))
OFFS = ((0, 128, 256), (384, 416, 448), (480, 488, 496))


def dot_nn(a, b):
    return lax.dot_general(a, b, (((1,), (0,)), ((), ())), preferred_element_type=F32)


def dot_nt(a, b):
    return lax.dot_general(a, b, (((1,), (1,)), ((), ())), preferred_element_type=F32)


def dot_tn(a, b):
    return lax.dot_general(a, b, (((0,), (0,)), ((), ())), preferred_element_type=F32)


def gelu_and_slope(pre):
    cdf = 0.5 * (1.0 + lax.erf(pre * INV_ROOT_TWO))
    return pre * cdf, cdf + pre * jnp.exp(-0.5 * pre * pre) * INV_ROOT_TWO_PI


def gelu(pre):
    return pre * (0.5 * (1.0 + lax.erf(pre * INV_ROOT_TWO)))


def kernel(x_hbm, g_hbm, w1_hbm, w2_hbm, w3_hbm, w4_hbm,
           gb, h2,
           xv, gv, w1, w2, w3, w4, a1, dh2, da, hc,
           drb, rbuf,
           in_sem, rsem, ssem, dsem_s, dsem_r):
    z, y, x = lax.axis_index('z'), lax.axis_index('y'), lax.axis_index('x')
    core = lax.rem(x, 2)
    cx = lax.div(x, 2)
    partner = (z, y, x + 1 - 2 * core)

    def hot(d):
        return lax.div((2 - d) * (1 - d), 2), d * (2 - d), lax.div(d * (d - 1), 2)

    def pos(d):
        ox, oy, oz = hot(d)
        return cx * ox + y * oy + z * oz

    def nbr(d, e):
        ox, oy, oz = hot(d)
        return (lax.rem(z + e * oz + 4, 4), lax.rem(y + e * oy + 4, 4),
                lax.rem(cx + e * ox + 4, 4) * 2 + core)

    loads = []
    n = 0

    def load(src, dst):
        nonlocal n
        cp = pltpu.make_async_copy(src, dst, in_sem.at[n])
        cp.start()
        n += 1
        return cp

    ld_x = load(x_hbm, xv)
    ld_w1 = [load(w1_hbm.at[:, pl.ds(c * CB, CB)], w1.at[c]) for c in range(NB)]
    ld_w2 = [load(w2_hbm.at[pl.ds(c * CB, CB), :], w2.at[c]) for c in range(NB)]
    ld_w3 = [load(w3_hbm.at[:, pl.ds(c * CB, CB)], w3.at[c]) for c in range(NB)]
    ld_g = load(g_hbm, gv)
    ld_w4 = [load(w4_hbm.at[pl.ds(c * CB, CB), :], w4.at[c]) for c in range(NB)]

    barrier = pltpu.get_barrier_semaphore()
    peers = [partner] + [nbr(d, e) for d in range(3) for e in (1, -1, 2)]
    for peer in peers:
        pl.semaphore_signal(barrier, inc=1, device_id=peer, device_id_type=MESH)
    pl.semaphore_wait(barrier, len(peers))

    ld_x.wait()
    for cp in ld_w1 + ld_w2:
        cp.wait()

    def fwd1(t, carry):
        rows = pl.ds(pl.multiple_of(t * TT, TT), TT)
        xt = xv[rows, :]
        acc = xt.astype(F32)
        for c in range(NB):
            pre = dot_nn(xt, w1[c]).astype(BF16)
            a1[c, rows, :] = pre
            acc = acc + dot_nn(gelu(pre.astype(F32)).astype(BF16), w2[c])
        h2[rows, :] = acc.astype(BF16)
        return carry

    lax.fori_loop(0, NT, fwd1, 0)
    for cp in ld_w3 + [ld_g] + ld_w4:
        cp.wait()

    def group(q, gi):
        u0, s = GROUPS[gi]
        rot = lax.rem(q + gi, 3)
        e = 1 - 2 * lax.rem(q + gi, 2)
        dims = [lax.rem(rot + k, 3) for k in range(3)]
        ps = [pos(d) for d in dims]
        base = [0, ps[0] * ROWS[0], ps[0] * ROWS[0] + ps[1] * ROWS[1]]
        return u0, s, e, dims, ps, base

    def piece(q, half, u0, s, start, length):
        return gb.at[q, half, pl.ds(u0, s), pl.ds(pl.multiple_of(start, 8), length), :]

    def rb(slot, u0, s, off, length):
        return rbuf.at[slot, pl.ds(u0, s), pl.ds(off, length), :]

    class Phase:
        def __init__(self, q, gi, k):
            self.u0, self.s, self.e, dims, ps, base = group(q, gi)
            self.q, self.gi, self.k = q, gi, k
            self.d, self.p, self.base = dims[k], ps[k], base[k]
            self.L = ROWS[k]
            self.slot = lax.rem(q, SL)
            self.dslot = lax.rem(q, ND)

        def rows(self, j):
            return self.base + lax.rem(self.p + j + 4, 4) * self.L

        def mine(self, j):
            return piece(self.q, core, self.u0, self.s, self.rows(j), self.L)

        def part(self, j):
            return drb.at[self.dslot, pl.ds(self.u0, self.s), pl.ds(pl.multiple_of(self.rows(j), 8), self.L), :]

        def pval(self, j):
            return (self.dslot, pl.ds(self.u0, self.s), pl.ds(pl.multiple_of(self.rows(j), 8), self.L), slice(None))

        def val(self, j):
            return (self.q, core, pl.ds(self.u0, self.s), pl.ds(pl.multiple_of(self.rows(j), 8), self.L), slice(None))

        def buf(self, i):
            return rb(self.slot, self.u0, self.s, OFFS[self.k][i], self.L)

        def bufval(self, i):
            return rbuf[self.slot, pl.ds(self.u0, self.s), pl.ds(OFFS[self.k][i], self.L), :]

        def copy(self, src, dst, i, toward):
            idx = self.k * 6 + i
            return pltpu.make_async_remote_copy(
                src_ref=src, dst_ref=dst, send_sem=ssem.at[self.slot, self.gi, idx],
                recv_sem=rsem.at[self.slot, self.gi, idx],
                device_id=nbr(self.d, toward), device_id_type=MESH)

        def far(self):
            return self.copy(self.part(2), self.buf(0), 0, 2 if DIRECT[self.k] else self.e)

        def near(self):
            return self.copy(self.part(-self.e), self.buf(1), 1, -self.e)

        def comb(self):
            return self.copy(self.part(self.e), self.buf(2), 2, self.e)

        def own_fwd(self):
            return self.copy(self.mine(0), self.mine(0), 3, self.e)

        def own_bwd(self):
            return self.copy(self.mine(0), self.mine(0), 4, -self.e)

        def relay(self):
            if DIRECT[self.k]:
                return self.copy(self.mine(0), self.mine(0), 5, 2)
            return self.copy(self.mine(-self.e), self.mine(-self.e), 5, self.e)

    def rs_a(q, k):
        for gi in range(3):
            ph = Phase(q, gi, k)
            ph.far().start()
            ph.near().start()
            if DIRECT[k]:
                ph.comb().start()

    def rs_b(q, k):
        for gi in range(3):
            ph = Phase(q, gi, k)
            ph.far().wait_recv()
            ix = ph.pval(ph.e)
            drb[ix] = drb[ix] + ph.bufval(0)
            ph.comb().start()

    def rs_c(q, k):
        for gi in range(3):
            ph = Phase(q, gi, k)
            ph.near().wait_recv()
            ph.comb().wait_recv()
            ix = ph.pval(0)
            tot = drb[ix] + (ph.bufval(1) + ph.bufval(2))
            if DIRECT[k]:
                ph.far().wait_recv()
                tot = tot + ph.bufval(0)
            if k == 2:
                gb[ph.val(0)] = tot * (1.0 / 128.0)
            else:
                drb[ix] = tot
            ph.far().wait_send()
            ph.near().wait_send()
            ph.comb().wait_send()

    def ag_a(q, k):
        for gi in range(3):
            ph = Phase(q, gi, k)
            ph.own_fwd().start()
            ph.own_bwd().start()
            if DIRECT[k]:
                ph.relay().start()

    def ag_b(q, k):
        for gi in range(3):
            ph = Phase(q, gi, k)
            ph.own_fwd().wait_recv()
            ph.relay().start()

    def ag_c(q, k):
        for gi in range(3):
            ph = Phase(q, gi, k)
            if DIRECT[k]:
                ph.own_fwd().wait_recv()
            ph.own_bwd().wait_recv()
            ph.relay().wait_recv()
            ph.own_fwd().wait_send()
            ph.own_bwd().wait_send()
            ph.relay().wait_send()

    def d2d(q, back):
        slot = lax.rem(q, SL)
        if back:
            src = dst = gb.at[q, core]
        else:
            src, dst = gb.at[q, 1 - core], drb.at[lax.rem(q, ND)]
        return pltpu.make_async_remote_copy(
            src_ref=src, dst_ref=dst, send_sem=dsem_s.at[slot, int(back)], recv_sem=dsem_r.at[slot, int(back)],
            device_id=partner, device_id_type=MESH)

    def start_pair(q):
        d2d(q, False).start()

    def finish_pair(q):
        d2d(q, False).wait_recv()
        slot = lax.rem(q, ND)
        drb[slot] = gb[q, core] + drb[slot]
        d2d(q, False).wait_send()

    def start_back(q):
        d2d(q, True).start()

    def finish_back(q):
        d2d(q, True).wait_recv()
        d2d(q, True).wait_send()

    stages = [[start_pair]]
    cur = [finish_pair]
    for k in (0, 1, 2):
        stages.append(cur + [functools.partial(rs_a, k=k)])
        if not DIRECT[k]:
            stages.append([functools.partial(rs_b, k=k)])
        cur = [functools.partial(rs_c, k=k)]
    for k in (2, 1, 0):
        stages.append(cur + [functools.partial(ag_a, k=k)])
        if not DIRECT[k]:
            stages.append([functools.partial(ag_b, k=k)])
        cur = [functools.partial(ag_c, k=k)]
    stages.append(cur + [start_back])
    stages.append([finish_back])
    when = [PER - 1 + DIST * s for s in range(len(stages))]
    n_iter = NQ + when[-1] // PER

    def tick(i, j):
        for s in reversed(range(len(stages))):
            if when[s] % PER == j:
                q = i - when[s] // PER

                @pl.when((q >= 0) & (q < NQ))
                def _():
                    for f in stages[s]:
                        f(q)

    def tile2(c, lo, hi):
        def body(t, carry):
            rows = pl.ds(pl.multiple_of(t * TT, TT), TT)
            pre = dot_nn(h2[rows, :], w3[c]).astype(BF16).astype(F32)
            act, slope = gelu_and_slope(pre)
            hc[rows, :] = act.astype(BF16)
            up = dot_nt(gv[rows, :], w4[c]).astype(BF16).astype(F32)
            da[c, rows, :] = (up * slope).astype(BF16)
            return carry
        lax.fori_loop(lo, hi, body, 0)

    def tile1(c, lo, hi):
        def body(t, carry):
            rows = pl.ds(pl.multiple_of(t * TT, TT), TT)
            pre = a1[c, rows, :].astype(F32)
            act, slope = gelu_and_slope(pre)
            hc[rows, :] = act.astype(BF16)
            up = dot_nt(dh2[rows, :], w2[c]).astype(BF16).astype(F32)
            da[c, rows, :] = (up * slope).astype(BF16)
            return carry
        lax.fori_loop(lo, hi, body, 0)

    def wgrad(q, c, down_rhs, up_lhs):
        down = dot_tn(hc[...], down_rhs[...])
        for u in range(4):
            gb[q, 0, u] = down[:, u * 128:(u + 1) * 128]
        up = dot_tn(up_lhs[...], da[c])
        for u in range(4):
            gb[q, 1, u] = up[:, u * 128:(u + 1) * 128]

    def back_tile(t, w, res, dst):
        rows = pl.ds(pl.multiple_of(t * TT, TT), TT)
        acc = res[rows, :].astype(F32)
        for c in range(NB):
            acc = acc + dot_nt(da[c, rows, :], w[c])
        dst[rows, :] = acc.astype(BF16)

    def back_all(i):
        @pl.when(i == NB)
        def _():
            def body(t, c):
                back_tile(t, w3, gv, dh2)
                return c
            lax.fori_loop(0, NT, body, 0)

    def step(i, carry):
        back_all(i)

        @pl.when((i >= NQ) & (i < NQ + NT))
        def _():
            back_tile(i - NQ, w1, dh2, h2)

        def part(j, c):
            lo, hi = j * (NT // (PER - 1)), (j + 1) * (NT // (PER - 1))

            @pl.when(i < NB)
            def _():
                tile2(i, lo, hi)

            @pl.when((i >= NB) & (i < NQ))
            def _():
                tile1(i - NB, lo, hi)

            for jj in range(PER - 1):
                @pl.when(j == jj)
                def _():
                    tick(i, jj)
            return c

        lax.fori_loop(0, PER - 1, part, 0)

        @pl.when(i < NB)
        def _():
            wgrad(i, i, gv, h2)

        @pl.when((i >= NB) & (i < NQ))
        def _():
            wgrad(i, i - NB, dh2, xv)

        tick(i, PER - 1)
        return carry

    lax.fori_loop(0, n_iter, step, 0)


def finish(gb, dx, o1, o2, o3, o4, odx, sem):
    copies = [pltpu.make_async_copy(dx, odx, sem.at[NQ * 8])]
    for q in range(NQ):
        down, up, c = (o4, o3, q) if q < NB else (o2, o1, q - NB)
        for u in range(4):
            cols = pl.ds(u * 128, 128)
            copies.append(pltpu.make_async_copy(gb.at[q, 0, u], down.at[pl.ds(c * CB, CB), cols], sem.at[q * 8 + u]))
            cols = pl.ds(c * CB + u * 128, 128)
            copies.append(pltpu.make_async_copy(gb.at[q, 1, u], up.at[:, cols], sem.at[q * 8 + 4 + u]))
    for cp in copies:
        cp.start()
    for cp in copies:
        cp.wait()


def solution(mesh):
    batch_spec = P(('z', 'y', 'x'), None)
    full_spec = P(None, None)

    def per_device(acts_in, grad_out, w_up1, w_down1, w_up2, w_down2):
        any_spec = pl.BlockSpec(memory_space=pl.ANY)
        up = jax.ShapeDtypeStruct((DM, FF), F32)
        down = jax.ShapeDtypeStruct((FF, DM), F32)
        vm_spec = pl.BlockSpec(memory_space=pltpu.VMEM)
        grads, dx = pl.pallas_call(
            kernel,
            out_shape=(pltpu.VMEM((NQ, 2, 4, 512, 128), F32), pltpu.VMEM((TOK, DM), BF16)),
            in_specs=[any_spec] * 6,
            out_specs=(vm_spec, vm_spec),
            scratch_shapes=[
                pltpu.VMEM((TOK, DM), BF16),
                pltpu.VMEM((TOK, DM), BF16),
                pltpu.VMEM((NB, DM, CB), BF16),
                pltpu.VMEM((NB, CB, DM), BF16),
                pltpu.VMEM((NB, DM, CB), BF16),
                pltpu.VMEM((NB, CB, DM), BF16),
                pltpu.VMEM((NB, TOK, CB), BF16),
                pltpu.VMEM((TOK, DM), BF16),
                pltpu.VMEM((NB, TOK, CB), BF16),
                pltpu.VMEM((TOK, CB), BF16),
                pltpu.VMEM((ND, 4, 512, 128), F32),
                pltpu.VMEM((SL, 4, 504, 128), F32),
                pltpu.SemaphoreType.DMA((18,)),
                pltpu.SemaphoreType.DMA((SL, 3, 18)),
                pltpu.SemaphoreType.DMA((SL, 3, 18)),
                pltpu.SemaphoreType.DMA((SL, 2)),
                pltpu.SemaphoreType.DMA((SL, 2)),
            ],
            compiler_params=pltpu.CompilerParams(
                collective_id=0, has_side_effects=True, vmem_limit_bytes=int(45.5 * 2**20)),
            cost_estimate=pl.CostEstimate(flops=12 * 2 * TOK * DM * FF, bytes_accessed=32 * 2**20, transcendentals=0),
        )(acts_in, grad_out, w_up1, w_down1, w_up2, w_down2)
        return pl.pallas_call(
            finish,
            out_shape=(up, down, up, down, jax.ShapeDtypeStruct((TOK, DM), BF16)),
            in_specs=[vm_spec, vm_spec],
            out_specs=(any_spec,) * 5,
            scratch_shapes=[pltpu.SemaphoreType.DMA((NQ * 8 + 1,))],
            compiler_params=pltpu.CompilerParams(vmem_limit_bytes=2**20),
        )(grads, dx)

    return jax.shard_map(per_device, mesh=mesh, in_specs=(batch_spec, batch_spec, full_spec, full_spec, full_spec, full_spec), out_specs=(full_spec, full_spec, full_spec, full_spec, batch_spec), check_vma=False)
```

```python
import functools
import math
import jax
import jax.numpy as jnp
from jax import lax
from jax.experimental import pallas as pl
from jax.experimental.pallas import tpu as pltpu
from jax.sharding import PartitionSpec as P

INV_ROOT_TWO = 1.0 / math.sqrt(2.0)
INV_ROOT_TWO_PI = 1.0 / math.sqrt(2.0 * math.pi)
HALF_LOG2_E = 0.5 / math.log(2.0)
SLOT3 = (0, 1, 2)
TAIL = (-1, -1, 7, 6, 5, 4, 3, 2, 1, -1, -1, 7, 6, 5, 4, 0, 3, 7, 6, 5, 2, 4, 7, 6, 5, 3, 2, 1, 7, 6, 4, 5, 7, 3, 6, 2, 4, 3, 5, 7, 6, 4, 5, 7, 5, 6, 7, 6, 7)
LOGICAL = pl.DeviceIdType.LOGICAL
BF16 = jnp.bfloat16
F32 = jnp.float32

TOK, DM, FF = 2048, 512, 2048
NB = 4
CB = FF // NB
NQ = 2 * NB
TT = 512
NT = TOK // TT
ND = 5
SL = 3
PER, DIST = 4, 3
DIRECT = (False, True, True)
ROWS = (128, 32, 8)
OUTER = ((0, 1, 0, 1), (1, 1, 0, 3), (2, 1, 1, 1), (3, 1, 2, 3))
INNER = ((0, 2, 0, 1), (2, 1, 1, 1), (3, 1, 2, 1))
OFFS = ((0, 128, 256), (384, 416, 448), (480, 488, 496))


def dot_nn(a, b):
    return lax.dot_general(a, b, (((1,), (0,)), ((), ())), preferred_element_type=F32)


def dot_nt(a, b):
    return lax.dot_general(a, b, (((1,), (1,)), ((), ())), preferred_element_type=F32)


def dot_tn(a, b):
    return lax.dot_general(a, b, (((0,), (0,)), ((), ())), preferred_element_type=F32)


def gelu_and_slope(pre):
    cdf = 0.5 * (1.0 + lax.erf(pre * INV_ROOT_TWO))
    return pre * cdf, cdf + pre * jnp.exp2(pre * pre * -HALF_LOG2_E) * INV_ROOT_TWO_PI


def gelu(pre):
    return pre * (0.5 * (1.0 + lax.erf(pre * INV_ROOT_TWO)))


def kernel(x_hbm, g_hbm, w1_hbm, w2_hbm, w3_hbm, w4_hbm,
           gb, h2,
           xv, gv, w1, w2, w3, w4, a1, dh2, da, hc,
           drb, rbuf,
           in_sem, rsem, ssem, dsem_s, dsem_r):
    z, y, x = lax.axis_index('z'), lax.axis_index('y'), lax.axis_index('x')
    core = lax.rem(x, 2)
    cx = lax.div(x, 2)
    me = z * 32 + y * 8 + x
    partner = me + 1 - 2 * core
    at = [[lax.rem(p + j, 4) for p in (cx, y, z)] for j in range(4)]
    dev = [[me + (at[j][d] - at[0][d]) * stride for d, stride in enumerate((2, 8, 32))] for j in range(4)]

    loads = []
    n = 0

    def load(src, dst):
        nonlocal n
        cp = pltpu.make_async_copy(src, dst, in_sem.at[n])
        cp.start()
        n += 1
        return cp

    ld_x = load(x_hbm, xv)
    ld_w1 = [load(w1_hbm.at[:, pl.ds(c * CB, CB)], w1.at[c]) for c in range(NB)]
    ld_w2 = [load(w2_hbm.at[pl.ds(c * CB, CB), :], w2.at[c]) for c in range(NB)]
    barrier = pltpu.get_barrier_semaphore()
    peers = [partner] + [dev[j][d] for j in (1, 2, 3) for d in range(3)]
    for peer in peers:
        pl.semaphore_signal(barrier, inc=1, device_id=peer, device_id_type=LOGICAL)

    ld_x.wait()
    for cp in ld_w1 + ld_w2:
        cp.wait()
    ld_w3 = [load(w3_hbm.at[:, pl.ds(c * CB, CB)], w3.at[c]) for c in range(NB)]
    ld_g = load(g_hbm, gv)
    ld_w4 = [load(w4_hbm.at[pl.ds(c * CB, CB), :], w4.at[c]) for c in range(NB)]

    def fwd1(t, carry):
        rows = pl.ds(pl.multiple_of(t * TT, TT), TT)
        xt = xv[rows, :]
        acc = xt.astype(F32)
        for c in range(NB):
            pre = dot_nn(xt, w1[c]).astype(BF16)
            a1[c, rows, :] = pre
            acc = acc + dot_nn(gelu(pre.astype(F32)).astype(BF16), w2[c])
        h2[rows, :] = acc.astype(BF16)
        return carry

    lax.fori_loop(0, NT, fwd1, 0)
    for cp in ld_w3 + [ld_g] + ld_w4:
        cp.wait()
    pl.semaphore_wait(barrier, len(peers))

    class Chunk:
        def __init__(self, q, select, dslot):
            self.q, self.select, self.dslot = q, select, dslot
            self.slot = select(SLOT3, 0)

    def static_chunk(q):
        return Chunk(q, lambda v, c: v[(q + c) % 3], q % ND)

    def dynamic_chunks(i):
        r, r6 = lax.rem(i, 3), lax.rem(i, ND)
        is0, is1 = r == 0, r == 1
        memo = {}

        def select(v, c):
            key = (id(v), c % 3)
            if key not in memo:
                a, b, d = v[c % 3], v[(c + 1) % 3], v[(c + 2) % 3]
                memo[key] = (jnp.where(is0, a, jnp.where(is1, b, d)), v)
            return memo[key][0]

        for v in at + dev:
            for c in range(3):
                select(v, c)
        for c in range(3):
            select(SLOT3, c)

        def make(back):
            t = r6 + (-back) % ND
            return Chunk(i - back, lambda v, c: select(v, c - back), jnp.where(t >= ND, t - ND, t))
        return make

    class Phase:
        def __init__(self, ch, gi, k):
            self.u0, self.s, rot, self.e = (INNER if DIRECT[k] else OUTER)[gi]
            self.ch, self.gi, self.k, self.c = ch, gi, k, rot + k
            self.L = ROWS[k]
            self.base = 0
            for kk in range(k):
                self.base = self.base + ch.select(at[0], rot + kk) * ROWS[kk]

        def place(self, j):
            start = self.base + self.ch.select(at[j % 4], self.c) * self.L
            return pl.ds(pl.multiple_of(start, 8), self.L)

        def mine(self, j):
            return gb.at[self.ch.q, core, pl.ds(self.u0, self.s), self.place(j), :]

        def part(self, j):
            return drb.at[self.ch.dslot, pl.ds(self.u0, self.s), self.place(j), :]

        def pval(self, j):
            return (self.ch.dslot, pl.ds(self.u0, self.s), self.place(j), slice(None))

        def val(self, j):
            return (self.ch.q, core, pl.ds(self.u0, self.s), self.place(j), slice(None))

        def buf(self, i):
            return rbuf.at[self.ch.slot, pl.ds(self.u0, self.s), pl.ds(OFFS[self.k][i], self.L), :]

        def bufval(self, i):
            return rbuf[self.ch.slot, pl.ds(self.u0, self.s), pl.ds(OFFS[self.k][i], self.L), :]

        def copy(self, src, dst, i, toward):
            idx = self.k * 6 + i
            return pltpu.make_async_remote_copy(
                src_ref=src, dst_ref=dst, send_sem=ssem.at[self.ch.dslot, self.gi, idx],
                recv_sem=rsem.at[self.ch.dslot, self.gi, idx],
                device_id=self.ch.select(dev[toward % 4], self.c), device_id_type=LOGICAL)

        def far(self):
            return self.copy(self.part(2), self.buf(0), 0, 2 if DIRECT[self.k] else self.e)

        def near(self):
            return self.copy(self.part((4 - self.e)), self.buf(1), 1, (4 - self.e))

        def comb(self):
            return self.copy(self.part(self.e), self.buf(2), 2, self.e)

        def own_fwd(self):
            return self.copy(self.mine(0), self.mine(0), 3, self.e)

        def own_bwd(self):
            return self.copy(self.mine(0), self.mine(0), 4, (4 - self.e))

        def relay(self):
            if DIRECT[self.k]:
                return self.copy(self.mine(0), self.mine(0), 5, 2)
            return self.copy(self.mine((4 - self.e)), self.mine((4 - self.e)), 5, self.e)

    def rs_a(ch, k):
        for gi in range(3 if DIRECT[k] else 4):
            ph = Phase(ch, gi, k)
            ph.far().start()
            ph.near().start()
            if DIRECT[k]:
                ph.comb().start()

    def rs_b(ch, k):
        for gi in range(3 if DIRECT[k] else 4):
            ph = Phase(ch, gi, k)
            ph.far().wait_recv()
            ix = ph.pval(ph.e)
            drb[ix] = drb[ix] + ph.bufval(0)
            ph.comb().start()

    def rs_c(ch, k):
        for gi in range(3 if DIRECT[k] else 4):
            ph = Phase(ch, gi, k)
            ph.near().wait_recv()
            ph.comb().wait_recv()
            ix = ph.pval(0)
            tot = drb[ix] + (ph.bufval(1) + ph.bufval(2))
            if DIRECT[k]:
                ph.far().wait_recv()
                tot = tot + ph.bufval(0)
            if k == 2:
                gb[ph.val(0)] = tot * (1.0 / 128.0)
            else:
                drb[ix] = tot
            ph.far().wait_send()
            ph.near().wait_send()
            ph.comb().wait_send()

    def ag_a(ch, k):
        for gi in range(3 if DIRECT[k] else 4):
            ph = Phase(ch, gi, k)
            ph.own_fwd().start()
            ph.own_bwd().start()
            if DIRECT[k]:
                ph.relay().start()

    def ag_b(ch, k):
        for gi in range(3 if DIRECT[k] else 4):
            ph = Phase(ch, gi, k)
            ph.own_fwd().wait_recv()
            ph.relay().start()

    def ag_c(ch, k):
        for gi in range(3 if DIRECT[k] else 4):
            ph = Phase(ch, gi, k)
            if DIRECT[k]:
                ph.own_fwd().wait_recv()
            ph.own_bwd().wait_recv()
            ph.relay().wait_recv()
            ph.own_fwd().wait_send()
            ph.own_bwd().wait_send()
            ph.relay().wait_send()

    def d2d(ch, back):
        if back:
            src = dst = gb.at[ch.q, core]
        else:
            src, dst = gb.at[ch.q, 1 - core], drb.at[ch.dslot]
        return pltpu.make_async_remote_copy(
            src_ref=src, dst_ref=dst, send_sem=dsem_s.at[ch.dslot, int(back)], recv_sem=dsem_r.at[ch.dslot, int(back)],
            device_id=partner, device_id_type=LOGICAL)

    def start_pair(ch):
        d2d(ch, False).start()

    def finish_pair(ch):
        d2d(ch, False).wait_recv()
        drb[ch.dslot] = gb[ch.q, core] + drb[ch.dslot]
        d2d(ch, False).wait_send()

    def start_back(ch):
        d2d(ch, True).start()

    def finish_back(ch):
        d2d(ch, True).wait_recv()
        d2d(ch, True).wait_send()

    stages = [[start_pair]]
    cur = [finish_pair]
    for k in (0, 1, 2):
        stages.append(cur + [functools.partial(rs_a, k=k)])
        if not DIRECT[k]:
            stages.append([functools.partial(rs_b, k=k)])
        cur = [functools.partial(rs_c, k=k)]
    for k in (2, 1, 0):
        stages.append(cur + [functools.partial(ag_a, k=k)])
        if not DIRECT[k]:
            stages.append([functools.partial(ag_b, k=k)])
        cur = [functools.partial(ag_c, k=k)]
    stages.append(cur + [start_back])
    stages.append([finish_back])
    when = [PER - 1 + DIST * s for s in range(len(stages))]

    def tick(make, j, i):
        for s in reversed(range(len(stages))):
            if when[s] % PER == j:
                back = when[s] // PER

                @pl.when((i >= back) if back else (i >= 0))
                def _():
                    ch = make(back)
                    for f in stages[s]:
                        f(ch)

    def tile2(c, t):
        rows = pl.ds(pl.multiple_of(t * TT, TT), TT)
        pre = dot_nn(h2[rows, :], w3[c]).astype(BF16).astype(F32)
        act, slope = gelu_and_slope(pre)
        hc[lax.rem(c, 2), rows, :] = act.astype(BF16)
        up = dot_nt(gv[rows, :], w4[c]).astype(BF16).astype(F32)
        da[c, rows, :] = (up * slope).astype(BF16)

    def tile1(c, t):
        rows = pl.ds(pl.multiple_of(t * TT, TT), TT)
        pre = a1[c, rows, :].astype(F32)
        act, slope = gelu_and_slope(pre)
        hc[lax.rem(c, 2), rows, :] = act.astype(BF16)
        up = dot_nt(dh2[rows, :], w2[c]).astype(BF16).astype(F32)
        da[c, rows, :] = (up * slope).astype(BF16)

    def wgrad(q, c, half, n, down_rhs, up_lhs):
        cols = pl.ds(pl.multiple_of(n * 256, 256), 256)
        if half == 0:
            prod = dot_tn(hc[lax.rem(c, 2)], down_rhs[:, cols])
        else:
            prod = dot_tn(up_lhs[...], da[c, :, cols])
        for u in range(2):
            gb[q, half, n * 2 + u] = prod[:, u * 128:(u + 1) * 128]

    def back_tile(t, w, res, dst):
        rows = pl.ds(t * TT if isinstance(t, int) else pl.multiple_of(t * TT, TT), TT)
        acc = res[rows, :].astype(F32)
        for c in range(NB):
            acc = acc + dot_nt(da[c, rows, :], w[c])
        dst[rows, :] = acc.astype(BF16)

    def step(i, carry):
        make = dynamic_chunks(i)

        @pl.when(i == NB)
        def _():
            def body(t, c):
                back_tile(t, w3, gv, dh2)
                tile1(0, t)
                return c
            lax.fori_loop(0, NT, body, 0)

        for half in range(2):
            def part(n, c):
                t = half * 2 + n

                @pl.when(i < NB - 1)
                def _():
                    wgrad(i, i, half, n, gv, h2)
                    tile2(i + 1, t)

                @pl.when(i == NB - 1)
                def _():
                    wgrad(i, i, half, n, gv, h2)

                @pl.when((i >= NB) & (i < NQ - 1))
                def _():
                    wgrad(i, i - NB, half, n, dh2, xv)
                    tile1(i - NB + 1, t)

                @pl.when(i == NQ - 1)
                def _():
                    wgrad(i, i - NB, half, n, dh2, xv)

                for jj in range(2):
                    @pl.when(n == jj)
                    def _():
                        tick(make, half * 2 + jj, i)
                return c

            lax.fori_loop(0, 2, part, 0)
        return carry

    def first(t, carry):
        tile2(0, t)
        return carry

    lax.fori_loop(0, NT, first, 0)
    lax.fori_loop(0, NQ, step, 0)

    done = [sum(w + PER * q < PER * NQ for w in when) for q in range(NQ)]
    tiles = 0
    for q in TAIL:
        if q < 0:
            back_tile(tiles, w1, dh2, h2)
            tiles += 1
        else:
            for f in stages[done[q]]:
                f(static_chunk(q))
            done[q] += 1
    assert tiles == NT and done == [len(stages)] * NQ


def finish(gb, dx, o1, o2, o3, o4, odx, sem):
    copies = [pltpu.make_async_copy(dx, odx, sem.at[NQ * 8])]
    for q in range(NQ):
        down, up, c = (o4, o3, q) if q < NB else (o2, o1, q - NB)
        for u in range(4):
            cols = pl.ds(u * 128, 128)
            copies.append(pltpu.make_async_copy(gb.at[q, 0, u], down.at[pl.ds(c * CB, CB), cols], sem.at[q * 8 + u]))
            cols = pl.ds(c * CB + u * 128, 128)
            copies.append(pltpu.make_async_copy(gb.at[q, 1, u], up.at[:, cols], sem.at[q * 8 + 4 + u]))
    for cp in copies:
        cp.start()
    for cp in copies:
        cp.wait()


def solution(mesh):
    batch_spec = P(('z', 'y', 'x'), None)
    full_spec = P(None, None)

    def per_device(acts_in, grad_out, w_up1, w_down1, w_up2, w_down2):
        any_spec = pl.BlockSpec(memory_space=pl.ANY)
        up = jax.ShapeDtypeStruct((DM, FF), F32)
        down = jax.ShapeDtypeStruct((FF, DM), F32)
        vm_spec = pl.BlockSpec(memory_space=pltpu.VMEM)
        grads, dx = pl.pallas_call(
            kernel,
            out_shape=(pltpu.VMEM((NQ, 2, 4, 512, 128), F32), pltpu.VMEM((TOK, DM), BF16)),
            in_specs=[any_spec] * 6,
            out_specs=(vm_spec, vm_spec),
            scratch_shapes=[
                pltpu.VMEM((TOK, DM), BF16),
                pltpu.VMEM((TOK, DM), BF16),
                pltpu.VMEM((NB, DM, CB), BF16),
                pltpu.VMEM((NB, CB, DM), BF16),
                pltpu.VMEM((NB, DM, CB), BF16),
                pltpu.VMEM((NB, CB, DM), BF16),
                pltpu.VMEM((NB, TOK, CB), BF16),
                pltpu.VMEM((TOK, DM), BF16),
                pltpu.VMEM((NB, TOK, CB), BF16),
                pltpu.VMEM((2, TOK, CB), BF16),
                pltpu.VMEM((ND, 4, 512, 128), F32),
                pltpu.VMEM((SL, 4, 504, 128), F32),
                pltpu.SemaphoreType.DMA((18,)),
                pltpu.SemaphoreType.DMA((ND, 4, 18)),
                pltpu.SemaphoreType.DMA((ND, 4, 18)),
                pltpu.SemaphoreType.DMA((ND, 2)),
                pltpu.SemaphoreType.DMA((ND, 2)),
            ],
            compiler_params=pltpu.CompilerParams(
                collective_id=0, has_side_effects=True, vmem_limit_bytes=int(45.9 * 2**20)),
            cost_estimate=pl.CostEstimate(flops=12 * 2 * TOK * DM * FF, bytes_accessed=32 * 2**20, transcendentals=0),
        )(acts_in, grad_out, w_up1, w_down1, w_up2, w_down2)
        return pl.pallas_call(
            finish,
            out_shape=(up, down, up, down, jax.ShapeDtypeStruct((TOK, DM), BF16)),
            in_specs=[vm_spec, vm_spec],
            out_specs=(any_spec,) * 5,
            scratch_shapes=[pltpu.SemaphoreType.DMA((NQ * 8 + 1,))],
            compiler_params=pltpu.CompilerParams(vmem_limit_bytes=2**20),
        )(grads, dx)

    return jax.shard_map(per_device, mesh=mesh, in_specs=(batch_spec, batch_spec, full_spec, full_spec, full_spec, full_spec), out_specs=(full_spec, full_spec, full_spec, full_spec, batch_spec), check_vma=False)
```

```python
import functools
import math
import jax
import jax.numpy as jnp
from jax import lax
from jax.experimental import pallas as pl
from jax.experimental.pallas import tpu as pltpu
from jax.sharding import PartitionSpec as P

INV_ROOT_TWO = 1.0 / math.sqrt(2.0)
INV_ROOT_TWO_PI = 1.0 / math.sqrt(2.0 * math.pi)
HALF_LOG2_E = 0.5 / math.log(2.0)
SLOT3 = (0, 1, 2)
TAIL = (-1, -1, 7, 6, 5, 4, 3, 2, 1, -1, -1, 7, 6, 5, 4, 0, 3, 7, 6, 5, 2, 4, 7, 6, 5, 3, 2, 1, 7, 6, 4, 5, 7, 3, 6, 2, 4, 3, 5, 7, 6, 4, 5, 7, 5, 6, 7, 6, 7)
LOGICAL = pl.DeviceIdType.LOGICAL
BF16 = jnp.bfloat16
F32 = jnp.float32

TOK, DM, FF = 2048, 512, 2048
NB = 4
CB = FF // NB
NQ = 2 * NB
TT = 512
NT = TOK // TT
ND = 5
SL = 3
PER, DIST = 4, 3
DIRECT = (False, True, True)
ROWS = (128, 32, 8)
OUTER = ((0, 1, 0, 1), (1, 1, 0, 3), (2, 1, 1, 1), (3, 1, 2, 3))
INNER = ((0, 2, 0, 1), (2, 1, 1, 1), (3, 1, 2, 1))
OFFS = ((0, 128, 256), (384, 416, 448), (480, 488, 496))


def dot_nn(a, b):
    return lax.dot_general(a, b, (((1,), (0,)), ((), ())), preferred_element_type=F32)


def dot_nt(a, b):
    return lax.dot_general(a, b, (((1,), (1,)), ((), ())), preferred_element_type=F32)


def dot_tn(a, b):
    return lax.dot_general(a, b, (((0,), (0,)), ((), ())), preferred_element_type=F32)


def gelu_and_slope(pre):
    cdf = 0.5 * (1.0 + lax.erf(pre * INV_ROOT_TWO))
    return pre * cdf, cdf + pre * jnp.exp2(pre * pre * -HALF_LOG2_E) * INV_ROOT_TWO_PI


def gelu(pre):
    return pre * (0.5 * (1.0 + lax.erf(pre * INV_ROOT_TWO)))


def kernel(x_hbm, g_hbm, w1_hbm, w2_hbm, w3_hbm, w4_hbm,
           gb, h2,
           xv, gv, w1, w2, w3, w4, a1, dh2, da, hc,
           drb, rbuf,
           in_sem, rsem, ssem, dsem_s, dsem_r):
    z, y, x = lax.axis_index('z'), lax.axis_index('y'), lax.axis_index('x')
    core = lax.rem(x, 2)
    cx = lax.div(x, 2)
    me = z * 32 + y * 8 + x
    partner = me + 1 - 2 * core
    at = [[lax.rem(p + j, 4) for p in (cx, y, z)] for j in range(4)]
    dev = [[me + (at[j][d] - at[0][d]) * stride for d, stride in enumerate((2, 8, 32))] for j in range(4)]

    loads = []
    n = 0

    def load(src, dst):
        nonlocal n
        cp = pltpu.make_async_copy(src, dst, in_sem.at[n])
        cp.start()
        n += 1
        return cp

    ld_x = load(x_hbm, xv)
    ld_w1 = [load(w1_hbm.at[:, pl.ds(c * CB, CB)], w1.at[c]) for c in range(NB)]
    ld_w2 = [load(w2_hbm.at[pl.ds(c * CB, CB), :], w2.at[c]) for c in range(NB)]
    barrier = pltpu.get_barrier_semaphore()
    peers = [partner] + [dev[j][d] for j in (1, 2, 3) for d in range(3)]
    for peer in peers:
        pl.semaphore_signal(barrier, inc=1, device_id=peer, device_id_type=LOGICAL)

    ld_x.wait()
    for cp in ld_w1 + ld_w2:
        cp.wait()
    ld_w3 = [load(w3_hbm.at[:, pl.ds(c * CB, CB)], w3.at[c]) for c in range(NB)]
    ld_g = load(g_hbm, gv)
    ld_w4 = [load(w4_hbm.at[pl.ds(c * CB, CB), :], w4.at[c]) for c in range(NB)]

    def fwd1(t, carry):
        rows = pl.ds(pl.multiple_of(t * TT, TT), TT)
        xt = xv[rows, :]
        acc = xt.astype(F32)
        for c in range(NB):
            pre = dot_nn(xt, w1[c]).astype(BF16)
            a1[c, rows, :] = pre
            acc = acc + dot_nn(gelu(pre.astype(F32)).astype(BF16), w2[c])
        h2[rows, :] = acc.astype(BF16)
        return carry

    lax.fori_loop(0, NT, fwd1, 0)
    for cp in ld_w3 + [ld_g] + ld_w4:
        cp.wait()
    pl.semaphore_wait(barrier, len(peers))

    class Chunk:
        def __init__(self, q, select, dslot):
            self.q, self.select, self.dslot = q, select, dslot
            self.slot = select(SLOT3, 0)

    def static_chunk(q):
        return Chunk(q, lambda v, c: v[(q + c) % 3], q % ND)

    def dynamic_chunks(i):
        r, r6 = lax.rem(i, 3), lax.rem(i, ND)
        is0, is1 = r == 0, r == 1
        memo = {}

        def select(v, c):
            key = (id(v), c % 3)
            if key not in memo:
                a, b, d = v[c % 3], v[(c + 1) % 3], v[(c + 2) % 3]
                memo[key] = (jnp.where(is0, a, jnp.where(is1, b, d)), v)
            return memo[key][0]

        for v in at + dev:
            for c in range(3):
                select(v, c)
        for c in range(3):
            select(SLOT3, c)

        def make(back):
            t = r6 + (-back) % ND
            return Chunk(i - back, lambda v, c: select(v, c - back), jnp.where(t >= ND, t - ND, t))
        return make

    class Phase:
        def __init__(self, ch, gi, k):
            self.u0, self.s, rot, self.e = (INNER if DIRECT[k] else OUTER)[gi]
            self.ch, self.gi, self.k, self.c = ch, gi, k, rot + k
            self.L = ROWS[k]
            self.base = 0
            for kk in range(k):
                self.base = self.base + ch.select(at[0], rot + kk) * ROWS[kk]

        def place(self, j):
            start = self.base + self.ch.select(at[j % 4], self.c) * self.L
            return pl.ds(pl.multiple_of(start, 8), self.L)

        def mine(self, j):
            return gb.at[self.ch.q, core, pl.ds(self.u0, self.s), self.place(j), :]

        def part(self, j):
            return drb.at[self.ch.dslot, pl.ds(self.u0, self.s), self.place(j), :]

        def pval(self, j):
            return (self.ch.dslot, pl.ds(self.u0, self.s), self.place(j), slice(None))

        def val(self, j):
            return (self.ch.q, core, pl.ds(self.u0, self.s), self.place(j), slice(None))

        def buf(self, i):
            return rbuf.at[self.ch.slot, pl.ds(self.u0, self.s), pl.ds(OFFS[self.k][i], self.L), :]

        def bufval(self, i):
            return rbuf[self.ch.slot, pl.ds(self.u0, self.s), pl.ds(OFFS[self.k][i], self.L), :]

        def copy(self, src, dst, i, toward):
            back = int(i >= 3)
            if DIRECT[self.k]:
                pair = ((self.k - 1) * 3 + self.gi) * 2 + back
                si, ri = 8 + pair, 16 + pair
            else:
                si, ri = self.gi * 2 + back, self.gi * 4 + (0, 1, 1, 2, 3, 3)[i]
            return pltpu.make_async_remote_copy(
                src_ref=src, dst_ref=dst, send_sem=ssem.at[self.ch.dslot, si], recv_sem=rsem.at[self.ch.dslot, ri],
                device_id=self.ch.select(dev[toward % 4], self.c), device_id_type=LOGICAL)

        def whole(self, i, pieces):
            ref = rbuf.at[self.ch.slot, pl.ds(self.u0, self.s), pl.ds(OFFS[self.k][0], pieces * self.L), :]
            return self.copy(ref, ref, i, 1)

        def far(self):
            return self.copy(self.part(2), self.buf(0), 0, 2 if DIRECT[self.k] else self.e)

        def near(self):
            return self.copy(self.part((4 - self.e)), self.buf(1), 1, (4 - self.e))

        def comb(self):
            return self.copy(self.part(self.e), self.buf(2), 2, self.e)

        def own_fwd(self):
            return self.copy(self.mine(0), self.mine(0), 3, self.e)

        def own_bwd(self):
            return self.copy(self.mine(0), self.mine(0), 4, (4 - self.e))

        def relay(self):
            if DIRECT[self.k]:
                return self.copy(self.mine(0), self.mine(0), 5, 2)
            return self.copy(self.mine((4 - self.e)), self.mine((4 - self.e)), 5, self.e)

    def rs_a(ch, k):
        for gi in range(3 if DIRECT[k] else 4):
            ph = Phase(ch, gi, k)
            ph.far().start()
            ph.near().start()
            if DIRECT[k]:
                ph.comb().start()

    def rs_b(ch, k):
        for gi in range(3 if DIRECT[k] else 4):
            ph = Phase(ch, gi, k)
            ph.far().wait_recv()
            ix = ph.pval(ph.e)
            drb[ix] = drb[ix] + ph.bufval(0)
            ph.comb().start()

    def rs_c(ch, k):
        for gi in range(3 if DIRECT[k] else 4):
            ph = Phase(ch, gi, k)
            if DIRECT[k]:
                ph.whole(0, 3).wait_recv()
            else:
                ph.whole(1, 2).wait_recv()
            ix = ph.pval(0)
            tot = drb[ix] + (ph.bufval(1) + ph.bufval(2))
            if DIRECT[k]:
                tot = tot + ph.bufval(0)
            if k == 2:
                gb[ph.val(0)] = tot * (1.0 / 128.0)
            else:
                drb[ix] = tot
            ph.whole(0, 3).wait_send()

    def ag_a(ch, k):
        for gi in range(3 if DIRECT[k] else 4):
            ph = Phase(ch, gi, k)
            ph.own_fwd().start()
            ph.own_bwd().start()
            if DIRECT[k]:
                ph.relay().start()

    def ag_b(ch, k):
        for gi in range(3 if DIRECT[k] else 4):
            ph = Phase(ch, gi, k)
            ph.own_fwd().wait_recv()
            ph.relay().start()

    def ag_c(ch, k):
        for gi in range(3 if DIRECT[k] else 4):
            ph = Phase(ch, gi, k)
            if DIRECT[k]:
                ph.whole(3, 3).wait_recv()
            else:
                ph.whole(4, 2).wait_recv()
            ph.whole(3, 3).wait_send()

    def d2d(ch, back):
        if back:
            src = dst = gb.at[ch.q, core]
        else:
            src, dst = gb.at[ch.q, 1 - core], drb.at[ch.dslot]
        return pltpu.make_async_remote_copy(
            src_ref=src, dst_ref=dst, send_sem=dsem_s.at[ch.dslot, int(back)], recv_sem=dsem_r.at[ch.dslot, int(back)],
            device_id=partner, device_id_type=LOGICAL)

    def start_pair(ch):
        d2d(ch, False).start()

    def finish_pair(ch):
        d2d(ch, False).wait_recv()
        drb[ch.dslot] = gb[ch.q, core] + drb[ch.dslot]
        d2d(ch, False).wait_send()

    def start_back(ch):
        d2d(ch, True).start()

    def finish_back(ch):
        d2d(ch, True).wait_recv()
        d2d(ch, True).wait_send()

    stages = [[start_pair]]
    cur = [finish_pair]
    for k in (0, 1, 2):
        stages.append(cur + [functools.partial(rs_a, k=k)])
        if not DIRECT[k]:
            stages.append([functools.partial(rs_b, k=k)])
        cur = [functools.partial(rs_c, k=k)]
    for k in (2, 1, 0):
        stages.append(cur + [functools.partial(ag_a, k=k)])
        if not DIRECT[k]:
            stages.append([functools.partial(ag_b, k=k)])
        cur = [functools.partial(ag_c, k=k)]
    stages.append(cur + [start_back])
    stages.append([finish_back])
    when = [PER - 1 + DIST * s for s in range(len(stages))]

    def tick(make, j, i):
        for s in reversed(range(len(stages))):
            if when[s] % PER == j:
                back = when[s] // PER

                @pl.when((i >= back) if back else (i >= 0))
                def _():
                    ch = make(back)
                    for f in stages[s]:
                        f(ch)

    def tile2(c, t):
        rows = pl.ds(pl.multiple_of(t * TT, TT), TT)
        pre = dot_nn(h2[rows, :], w3[c]).astype(BF16).astype(F32)
        act, slope = gelu_and_slope(pre)
        hc[lax.rem(c, 2), rows, :] = act.astype(BF16)
        up = dot_nt(gv[rows, :], w4[c]).astype(BF16).astype(F32)
        da[c, rows, :] = (up * slope).astype(BF16)

    def tile1(c, t):
        rows = pl.ds(pl.multiple_of(t * TT, TT), TT)
        pre = a1[c, rows, :].astype(F32)
        act, slope = gelu_and_slope(pre)
        hc[lax.rem(c, 2), rows, :] = act.astype(BF16)
        up = dot_nt(dh2[rows, :], w2[c]).astype(BF16).astype(F32)
        da[c, rows, :] = (up * slope).astype(BF16)

    def wgrad(q, c, half, n, down_rhs, up_lhs):
        cols = pl.ds(pl.multiple_of(n * 256, 256), 256)
        if half == 0:
            prod = dot_tn(hc[lax.rem(c, 2)], down_rhs[:, cols])
        else:
            prod = dot_tn(up_lhs[...], da[c, :, cols])
        for u in range(2):
            gb[q, half, n * 2 + u] = prod[:, u * 128:(u + 1) * 128]

    def back_tile(t, w, res, dst):
        rows = pl.ds(t * TT if isinstance(t, int) else pl.multiple_of(t * TT, TT), TT)
        acc = res[rows, :].astype(F32)
        for c in range(NB):
            acc = acc + dot_nt(da[c, rows, :], w[c])
        dst[rows, :] = acc.astype(BF16)

    def step(i, carry):
        make = dynamic_chunks(i)

        @pl.when(i == NB)
        def _():
            def body(t, c):
                back_tile(t, w3, gv, dh2)
                tile1(0, t)
                return c
            lax.fori_loop(0, NT, body, 0)

        for half in range(2):
            def part(n, c):
                t = half * 2 + n

                @pl.when(i < NB - 1)
                def _():
                    wgrad(i, i, half, n, gv, h2)
                    tile2(i + 1, t)

                @pl.when(i == NB - 1)
                def _():
                    wgrad(i, i, half, n, gv, h2)

                @pl.when((i >= NB) & (i < NQ - 1))
                def _():
                    wgrad(i, i - NB, half, n, dh2, xv)
                    tile1(i - NB + 1, t)

                @pl.when(i == NQ - 1)
                def _():
                    wgrad(i, i - NB, half, n, dh2, xv)

                for jj in range(2):
                    @pl.when(n == jj)
                    def _():
                        tick(make, half * 2 + jj, i)
                return c

            lax.fori_loop(0, 2, part, 0)
        return carry

    def first(t, carry):
        tile2(0, t)
        return carry

    lax.fori_loop(0, NT, first, 0)
    lax.fori_loop(0, NQ, step, 0)

    done = [sum(w + PER * q < PER * NQ for w in when) for q in range(NQ)]
    tiles = 0
    for q in TAIL:
        if q < 0:
            back_tile(tiles, w1, dh2, h2)
            tiles += 1
        else:
            for f in stages[done[q]]:
                f(static_chunk(q))
            done[q] += 1
    assert tiles == NT and done == [len(stages)] * NQ


def finish(gb, dx, o1, o2, o3, o4, odx, sem):
    pltpu.make_async_copy(dx, odx, sem.at[4]).start()
    for q in range(NQ):
        (down, ds), (up, us), c = ((o4, 3), (o3, 2), q) if q < NB else ((o2, 1), (o1, 0), q - NB)
        for u in range(4):
            cols = pl.ds(u * 128, 128)
            pltpu.make_async_copy(gb.at[q, 0, u], down.at[pl.ds(c * CB, CB), cols], sem.at[ds]).start()
            cols = pl.ds(c * CB + u * 128, 128)
            pltpu.make_async_copy(gb.at[q, 1, u], up.at[:, cols], sem.at[us]).start()
    for n, out in enumerate((o1, o2, o3, o4, odx)):
        pltpu.make_async_copy(out, out, sem.at[n]).wait()


def solution(mesh):
    batch_spec = P(('z', 'y', 'x'), None)
    full_spec = P(None, None)

    def per_device(acts_in, grad_out, w_up1, w_down1, w_up2, w_down2):
        any_spec = pl.BlockSpec(memory_space=pl.ANY)
        up = jax.ShapeDtypeStruct((DM, FF), F32)
        down = jax.ShapeDtypeStruct((FF, DM), F32)
        vm_spec = pl.BlockSpec(memory_space=pltpu.VMEM)
        grads, dx = pl.pallas_call(
            kernel,
            out_shape=(pltpu.VMEM((NQ, 2, 4, 512, 128), F32), pltpu.VMEM((TOK, DM), BF16)),
            in_specs=[any_spec] * 6,
            out_specs=(vm_spec, vm_spec),
            scratch_shapes=[
                pltpu.VMEM((TOK, DM), BF16),
                pltpu.VMEM((TOK, DM), BF16),
                pltpu.VMEM((NB, DM, CB), BF16),
                pltpu.VMEM((NB, CB, DM), BF16),
                pltpu.VMEM((NB, DM, CB), BF16),
                pltpu.VMEM((NB, CB, DM), BF16),
                pltpu.VMEM((NB, TOK, CB), BF16),
                pltpu.VMEM((TOK, DM), BF16),
                pltpu.VMEM((NB, TOK, CB), BF16),
                pltpu.VMEM((2, TOK, CB), BF16),
                pltpu.VMEM((ND, 4, 512, 128), F32),
                pltpu.VMEM((SL, 4, 504, 128), F32),
                pltpu.SemaphoreType.DMA((18,)),
                pltpu.SemaphoreType.DMA((ND, 28)),
                pltpu.SemaphoreType.DMA((ND, 20)),
                pltpu.SemaphoreType.DMA((ND, 2)),
                pltpu.SemaphoreType.DMA((ND, 2)),
            ],
            compiler_params=pltpu.CompilerParams(
                collective_id=0, has_side_effects=True, vmem_limit_bytes=int(45.9 * 2**20)),
            cost_estimate=pl.CostEstimate(flops=12 * 2 * TOK * DM * FF, bytes_accessed=32 * 2**20, transcendentals=0),
        )(acts_in, grad_out, w_up1, w_down1, w_up2, w_down2)
        return pl.pallas_call(
            finish,
            out_shape=(up, down, up, down, jax.ShapeDtypeStruct((TOK, DM), BF16)),
            in_specs=[vm_spec, vm_spec],
            out_specs=(any_spec,) * 5,
            scratch_shapes=[pltpu.SemaphoreType.DMA((5,))],
            compiler_params=pltpu.CompilerParams(vmem_limit_bytes=2**20),
        )(grads, dx)

    return jax.shard_map(per_device, mesh=mesh, in_specs=(batch_spec, batch_spec, full_spec, full_spec, full_spec, full_spec), out_specs=(full_spec, full_spec, full_spec, full_spec, batch_spec), check_vma=False)
```

```python
import functools
import math
import jax
import jax.numpy as jnp
from jax import lax
from jax.experimental import pallas as pl
from jax.experimental.pallas import tpu as pltpu
from jax.sharding import PartitionSpec as P

INV_ROOT_TWO = 1.0 / math.sqrt(2.0)
INV_ROOT_TWO_PI = 1.0 / math.sqrt(2.0 * math.pi)
HALF_LOG2_E = 0.5 / math.log(2.0)
SLOT3 = (0, 1, 2)
TAIL = (-1, -1, 7, 6, 5, 4, 3, 2, 1, -1, -1, 7, 6, 5, 4, 0, 3, 7, 6, 5, 2, 4, 7, 6, 5, 3, 2, 1, 7, 6, 4, 5, 7, 3, 6, 2, 4, 3, 5, 7, 6, 4, 5, 7, 5, 6, 7, 6, 7)
LOGICAL = pl.DeviceIdType.LOGICAL
BF16 = jnp.bfloat16
F32 = jnp.float32

TOK, DM, FF = 2048, 512, 2048
NB = 4
CB = FF // NB
NQ = 2 * NB
TT = 512
NT = TOK // TT
ND = 5
SL = 3
PER, DIST = 4, 3
DIRECT = (False, True, True)
ROWS = (128, 32, 8)
OUTER = ((0, 1, 0, 1), (1, 1, 0, 3), (2, 1, 1, 1), (3, 1, 2, 3))
INNER = ((0, 2, 0, 1), (2, 1, 1, 1), (3, 1, 2, 1))
OFFS = ((0, 128, 256), (384, 416, 448), (480, 488, 496))


def dot_nn(a, b):
    return lax.dot_general(a, b, (((1,), (0,)), ((), ())), preferred_element_type=F32)


def dot_nt(a, b):
    return lax.dot_general(a, b, (((1,), (1,)), ((), ())), preferred_element_type=F32)


def dot_tn(a, b):
    return lax.dot_general(a, b, (((0,), (0,)), ((), ())), preferred_element_type=F32)


def gelu_and_slope(pre):
    cdf = 0.5 * (1.0 + lax.erf(pre * INV_ROOT_TWO))
    return pre * cdf, cdf + pre * jnp.exp2(pre * pre * -HALF_LOG2_E) * INV_ROOT_TWO_PI


def gelu(pre):
    return pre * (0.5 * (1.0 + lax.erf(pre * INV_ROOT_TWO)))


def kernel(x_hbm, g_hbm, w1_hbm, w2_hbm, w3_hbm, w4_hbm,
           gb, h2,
           xv, gv, w1, w2, w3, w4, a1, dh2, da, hc,
           drb, rbuf,
           in_sem, rsem, ssem, dsem_s, dsem_r):
    z, y, x = lax.axis_index('z'), lax.axis_index('y'), lax.axis_index('x')
    core = lax.rem(x, 2)
    cx = lax.div(x, 2)
    me = z * 32 + y * 8 + x
    partner = me + 1 - 2 * core
    at = [[lax.rem(p + j, 4) for p in (cx, y, z)] for j in range(4)]
    dev = [[me + (at[j][d] - at[0][d]) * stride for d, stride in enumerate((2, 8, 32))] for j in range(4)]

    def load_blocks(n, hbm, vmem, by_rows):
        for c in range(NB):
            span = pl.ds(c * CB, CB)
            src = hbm.at[span, :] if by_rows else hbm.at[:, span]
            pltpu.make_async_copy(src, vmem.at[c], in_sem.at[n]).start()

    def load_wait(n, hbm):
        pltpu.make_async_copy(hbm, hbm, in_sem.at[n]).wait()

    pltpu.make_async_copy(x_hbm, xv, in_sem.at[0]).start()
    load_blocks(1, w1_hbm, w1, False)
    load_blocks(2, w2_hbm, w2, True)

    barrier = pltpu.get_barrier_semaphore()
    peers = [partner] + [dev[j][d] for j in (1, 2, 3) for d in range(3)]
    for peer in peers:
        pl.semaphore_signal(barrier, inc=1, device_id=peer, device_id_type=LOGICAL)

    for n, hbm in enumerate((x_hbm, w1_hbm, w2_hbm)):
        load_wait(n, hbm)
    load_blocks(3, w3_hbm, w3, False)
    pltpu.make_async_copy(g_hbm, gv, in_sem.at[4]).start()
    load_blocks(5, w4_hbm, w4, True)

    def fwd1(t, carry):
        rows = pl.ds(pl.multiple_of(t * TT, TT), TT)
        xt = xv[rows, :]
        acc = xt.astype(F32)
        for c in range(NB):
            pre = dot_nn(xt, w1[c]).astype(BF16)
            a1[c, rows, :] = pre
            acc = acc + dot_nn(gelu(pre.astype(F32)).astype(BF16), w2[c])
        h2[rows, :] = acc.astype(BF16)
        return carry

    lax.fori_loop(0, NT, fwd1, 0)
    for n, hbm in enumerate((w3_hbm, g_hbm, w4_hbm)):
        load_wait(n + 3, hbm)
    pl.semaphore_wait(barrier, len(peers))

    class Chunk:
        def __init__(self, q, select, dslot):
            self.q, self.select, self.dslot = q, select, dslot
            self.slot = select(SLOT3, 0)

    def static_chunk(q):
        return Chunk(q, lambda v, c: v[(q + c) % 3], q % ND)

    def dynamic_chunks(i):
        r, r6 = lax.rem(i, 3), lax.rem(i, ND)
        is0, is1 = r == 0, r == 1
        memo = {}

        def select(v, c):
            key = (id(v), c % 3)
            if key not in memo:
                a, b, d = v[c % 3], v[(c + 1) % 3], v[(c + 2) % 3]
                memo[key] = (jnp.where(is0, a, jnp.where(is1, b, d)), v)
            return memo[key][0]

        for v in at + dev:
            for c in range(3):
                select(v, c)
        for c in range(3):
            select(SLOT3, c)

        def make(back):
            t = r6 + (-back) % ND
            return Chunk(i - back, lambda v, c: select(v, c - back), jnp.where(t >= ND, t - ND, t))
        return make

    class Phase:
        def __init__(self, ch, gi, k):
            self.u0, self.s, rot, self.e = (INNER if DIRECT[k] else OUTER)[gi]
            self.ch, self.gi, self.k, self.c = ch, gi, k, rot + k
            self.L = ROWS[k]
            self.base = 0
            for kk in range(k):
                self.base = self.base + ch.select(at[0], rot + kk) * ROWS[kk]

        def place(self, j):
            start = self.base + self.ch.select(at[j % 4], self.c) * self.L
            return pl.ds(pl.multiple_of(start, 8), self.L)

        def mine(self, j):
            return gb.at[self.ch.q, core, pl.ds(self.u0, self.s), self.place(j), :]

        def part(self, j):
            return drb.at[self.ch.dslot, pl.ds(self.u0, self.s), self.place(j), :]

        def pval(self, j):
            return (self.ch.dslot, pl.ds(self.u0, self.s), self.place(j), slice(None))

        def val(self, j):
            return (self.ch.q, core, pl.ds(self.u0, self.s), self.place(j), slice(None))

        def buf(self, i):
            return rbuf.at[self.ch.slot, pl.ds(self.u0, self.s), pl.ds(OFFS[self.k][i], self.L), :]

        def bufval(self, i):
            return rbuf[self.ch.slot, pl.ds(self.u0, self.s), pl.ds(OFFS[self.k][i], self.L), :]

        def copy(self, src, dst, i, toward):
            back = int(i >= 3)
            if DIRECT[self.k]:
                pair = ((self.k - 1) * 3 + self.gi) * 2 + back
                si, ri = 8 + pair, 16 + pair
            else:
                si, ri = self.gi * 2 + back, self.gi * 4 + (0, 1, 1, 2, 3, 3)[i]
            return pltpu.make_async_remote_copy(
                src_ref=src, dst_ref=dst, send_sem=ssem.at[self.ch.dslot, si], recv_sem=rsem.at[self.ch.dslot, ri],
                device_id=self.ch.select(dev[toward % 4], self.c), device_id_type=LOGICAL)

        def whole(self, i, pieces):
            ref = rbuf.at[self.ch.slot, pl.ds(self.u0, self.s), pl.ds(OFFS[self.k][0], pieces * self.L), :]
            return self.copy(ref, ref, i, 1)

        def far(self):
            return self.copy(self.part(2), self.buf(0), 0, 2 if DIRECT[self.k] else self.e)

        def near(self):
            return self.copy(self.part((4 - self.e)), self.buf(1), 1, (4 - self.e))

        def comb(self):
            return self.copy(self.part(self.e), self.buf(2), 2, self.e)

        def own_fwd(self):
            return self.copy(self.mine(0), self.mine(0), 3, self.e)

        def own_bwd(self):
            return self.copy(self.mine(0), self.mine(0), 4, (4 - self.e))

        def relay(self):
            if DIRECT[self.k]:
                return self.copy(self.mine(0), self.mine(0), 5, 2)
            return self.copy(self.mine((4 - self.e)), self.mine((4 - self.e)), 5, self.e)

    def rs_a(ch, k):
        for gi in range(3 if DIRECT[k] else 4):
            ph = Phase(ch, gi, k)
            ph.far().start()
            ph.near().start()
            if DIRECT[k]:
                ph.comb().start()

    def rs_b(ch, k):
        for gi in range(3 if DIRECT[k] else 4):
            ph = Phase(ch, gi, k)
            ph.far().wait_recv()
            ix = ph.pval(ph.e)
            drb[ix] = drb[ix] + ph.bufval(0)
            ph.comb().start()

    def rs_c(ch, k):
        for gi in range(3 if DIRECT[k] else 4):
            ph = Phase(ch, gi, k)
            if DIRECT[k]:
                ph.whole(0, 3).wait_recv()
            else:
                ph.whole(1, 2).wait_recv()
            ix = ph.pval(0)
            tot = drb[ix] + (ph.bufval(1) + ph.bufval(2))
            if DIRECT[k]:
                tot = tot + ph.bufval(0)
            if k == 2:
                gb[ph.val(0)] = tot * (1.0 / 128.0)
            else:
                drb[ix] = tot
            ph.whole(0, 3).wait_send()

    def ag_a(ch, k):
        for gi in range(3 if DIRECT[k] else 4):
            ph = Phase(ch, gi, k)
            ph.own_fwd().start()
            ph.own_bwd().start()
            if DIRECT[k]:
                ph.relay().start()

    def ag_b(ch, k):
        for gi in range(3 if DIRECT[k] else 4):
            ph = Phase(ch, gi, k)
            ph.own_fwd().wait_recv()
            ph.relay().start()

    def ag_c(ch, k):
        for gi in range(3 if DIRECT[k] else 4):
            ph = Phase(ch, gi, k)
            if DIRECT[k]:
                ph.whole(3, 3).wait_recv()
            else:
                ph.whole(4, 2).wait_recv()
            ph.whole(3, 3).wait_send()

    def d2d(ch, back):
        if back:
            src = dst = gb.at[ch.q, core]
        else:
            src, dst = gb.at[ch.q, 1 - core], drb.at[ch.dslot]
        return pltpu.make_async_remote_copy(
            src_ref=src, dst_ref=dst, send_sem=dsem_s.at[ch.dslot, int(back)], recv_sem=dsem_r.at[ch.dslot, int(back)],
            device_id=partner, device_id_type=LOGICAL)

    def start_pair(ch):
        d2d(ch, False).start()

    def finish_pair(ch):
        d2d(ch, False).wait_recv()
        drb[ch.dslot] = gb[ch.q, core] + drb[ch.dslot]
        d2d(ch, False).wait_send()

    def start_back(ch):
        d2d(ch, True).start()

    def finish_back(ch):
        d2d(ch, True).wait_recv()
        d2d(ch, True).wait_send()

    stages = [[start_pair]]
    cur = [finish_pair]
    for k in (0, 1, 2):
        stages.append(cur + [functools.partial(rs_a, k=k)])
        if not DIRECT[k]:
            stages.append([functools.partial(rs_b, k=k)])
        cur = [functools.partial(rs_c, k=k)]
    for k in (2, 1, 0):
        stages.append(cur + [functools.partial(ag_a, k=k)])
        if not DIRECT[k]:
            stages.append([functools.partial(ag_b, k=k)])
        cur = [functools.partial(ag_c, k=k)]
    stages.append(cur + [start_back])
    stages.append([finish_back])
    when = [PER - 1 + DIST * s for s in range(len(stages))]

    def tick(make, j, i):
        for s in reversed(range(len(stages))):
            if when[s] % PER == j:
                back = when[s] // PER

                @pl.when((i >= back) if back else (i >= 0))
                def _():
                    ch = make(back)
                    for f in stages[s]:
                        f(ch)

    def tile2(c, t):
        rows = pl.ds(pl.multiple_of(t * TT, TT), TT)
        pre = dot_nn(h2[rows, :], w3[c]).astype(BF16).astype(F32)
        act, slope = gelu_and_slope(pre)
        hc[lax.rem(c, 2), rows, :] = act.astype(BF16)
        up = dot_nt(gv[rows, :], w4[c]).astype(BF16).astype(F32)
        da[c, rows, :] = (up * slope).astype(BF16)

    def tile1(c, t):
        rows = pl.ds(pl.multiple_of(t * TT, TT), TT)
        pre = a1[c, rows, :].astype(F32)
        act, slope = gelu_and_slope(pre)
        hc[lax.rem(c, 2), rows, :] = act.astype(BF16)
        up = dot_nt(dh2[rows, :], w2[c]).astype(BF16).astype(F32)
        da[c, rows, :] = (up * slope).astype(BF16)

    def wgrad(q, c, half, n, down_rhs, up_lhs):
        cols = pl.ds(pl.multiple_of(n * 256, 256), 256)
        if half == 0:
            prod = dot_tn(hc[lax.rem(c, 2)], down_rhs[:, cols])
        else:
            prod = dot_tn(up_lhs[...], da[c, :, cols])
        for u in range(2):
            gb[q, half, n * 2 + u] = prod[:, u * 128:(u + 1) * 128]

    def back_tile(t, w, res, dst):
        rows = pl.ds(t * TT if isinstance(t, int) else pl.multiple_of(t * TT, TT), TT)
        acc = res[rows, :].astype(F32)
        for c in range(NB):
            acc = acc + dot_nt(da[c, rows, :], w[c])
        dst[rows, :] = acc.astype(BF16)

    def step(i, carry):
        make = dynamic_chunks(i)

        @pl.when(i == NB)
        def _():
            def body(t, c):
                back_tile(t, w3, gv, dh2)
                tile1(0, t)
                return c
            lax.fori_loop(0, NT, body, 0)

        for half in range(2):
            def part(n, c):
                t = half * 2 + n

                @pl.when(i < NB - 1)
                def _():
                    wgrad(i, i, half, n, gv, h2)
                    tile2(i + 1, t)

                @pl.when(i == NB - 1)
                def _():
                    wgrad(i, i, half, n, gv, h2)

                @pl.when((i >= NB) & (i < NQ - 1))
                def _():
                    wgrad(i, i - NB, half, n, dh2, xv)
                    tile1(i - NB + 1, t)

                @pl.when(i == NQ - 1)
                def _():
                    wgrad(i, i - NB, half, n, dh2, xv)

                for jj in range(2):
                    @pl.when(n == jj)
                    def _():
                        tick(make, half * 2 + jj, i)
                return c

            lax.fori_loop(0, 2, part, 0)
        return carry

    def first(t, carry):
        tile2(0, t)
        return carry

    lax.fori_loop(0, NT, first, 0)
    lax.fori_loop(0, NQ, step, 0)

    done = [sum(w + PER * q < PER * NQ for w in when) for q in range(NQ)]
    tiles = 0
    for q in TAIL:
        if q < 0:
            back_tile(tiles, w1, dh2, h2)
            tiles += 1
        else:
            for f in stages[done[q]]:
                f(static_chunk(q))
            done[q] += 1
    assert tiles == NT and done == [len(stages)] * NQ


def finish(gb, dx, o1, o2, o3, o4, odx, sem):
    pltpu.make_async_copy(dx, odx, sem.at[4]).start()
    for q in range(NQ):
        (down, ds), (up, us), c = ((o4, 3), (o3, 2), q) if q < NB else ((o2, 1), (o1, 0), q - NB)
        for u in range(4):
            cols = pl.ds(u * 128, 128)
            pltpu.make_async_copy(gb.at[q, 0, u], down.at[pl.ds(c * CB, CB), cols], sem.at[ds]).start()
            cols = pl.ds(c * CB + u * 128, 128)
            pltpu.make_async_copy(gb.at[q, 1, u], up.at[:, cols], sem.at[us]).start()
    for n, out in enumerate((o1, o2, o3, o4, odx)):
        pltpu.make_async_copy(out, out, sem.at[n]).wait()


def solution(mesh):
    batch_spec = P(('z', 'y', 'x'), None)
    full_spec = P(None, None)

    def per_device(acts_in, grad_out, w_up1, w_down1, w_up2, w_down2):
        any_spec = pl.BlockSpec(memory_space=pl.ANY)
        up = jax.ShapeDtypeStruct((DM, FF), F32)
        down = jax.ShapeDtypeStruct((FF, DM), F32)
        vm_spec = pl.BlockSpec(memory_space=pltpu.VMEM)
        grads, dx = pl.pallas_call(
            kernel,
            out_shape=(pltpu.VMEM((NQ, 2, 4, 512, 128), F32), pltpu.VMEM((TOK, DM), BF16)),
            in_specs=[any_spec] * 6,
            out_specs=(vm_spec, vm_spec),
            scratch_shapes=[
                pltpu.VMEM((TOK, DM), BF16),
                pltpu.VMEM((TOK, DM), BF16),
                pltpu.VMEM((NB, DM, CB), BF16),
                pltpu.VMEM((NB, CB, DM), BF16),
                pltpu.VMEM((NB, DM, CB), BF16),
                pltpu.VMEM((NB, CB, DM), BF16),
                pltpu.VMEM((NB, TOK, CB), BF16),
                pltpu.VMEM((TOK, DM), BF16),
                pltpu.VMEM((NB, TOK, CB), BF16),
                pltpu.VMEM((2, TOK, CB), BF16),
                pltpu.VMEM((ND, 4, 512, 128), F32),
                pltpu.VMEM((SL, 4, 504, 128), F32),
                pltpu.SemaphoreType.DMA((6,)),
                pltpu.SemaphoreType.DMA((ND, 28)),
                pltpu.SemaphoreType.DMA((ND, 20)),
                pltpu.SemaphoreType.DMA((ND, 2)),
                pltpu.SemaphoreType.DMA((ND, 2)),
            ],
            compiler_params=pltpu.CompilerParams(
                collective_id=0, has_side_effects=True, vmem_limit_bytes=int(45.9 * 2**20)),
            cost_estimate=pl.CostEstimate(flops=12 * 2 * TOK * DM * FF, bytes_accessed=32 * 2**20, transcendentals=0),
        )(acts_in, grad_out, w_up1, w_down1, w_up2, w_down2)
        return pl.pallas_call(
            finish,
            out_shape=(up, down, up, down, jax.ShapeDtypeStruct((TOK, DM), BF16)),
            in_specs=[vm_spec, vm_spec],
            out_specs=(any_spec,) * 5,
            scratch_shapes=[pltpu.SemaphoreType.DMA((5,))],
            compiler_params=pltpu.CompilerParams(vmem_limit_bytes=2**20),
        )(grads, dx)

    return jax.shard_map(per_device, mesh=mesh, in_specs=(batch_spec, batch_spec, full_spec, full_spec, full_spec, full_spec), out_specs=(full_spec, full_spec, full_spec, full_spec, batch_spec), check_vma=False)
```
